32 devices in a mesh: groups: 2 (over x), seq: 16 (over z, y, core).
Axes of the slice: x: 2, y: 2, z: 4, core: 2. Of those that a mesh axis runs over, the one named last changes fastest.
Arguments:
- activations: bfloat16 [512, 14336], P(('groups', 'seq')), parts along dimension 0, may hold values from -6 to 6
- out_grads: bfloat16 [512, 2048], P(('groups', 'seq')), parts along dimension 0, may hold values from -6 to 6
- query_ids: int32 [512], P(('groups', 'seq')), parts along dimension 0, may hold values from 0 to 2, never falling along the last dimension, each value on 1 to 128 neighbouring positions
- act_basis: bfloat16 [64, 224, 224], P('seq'), may hold values from -0.375 to 0.375
- grad_basis: bfloat16 [2048, 2048], P(None, 'seq'), may hold values from -0.125 to 0.125
- eigenvalues: float32 [2048, 14336], P(None, 'seq'), may hold values from 8 to 80
Outputs:
- precond: bfloat16 [6, 2048, 14336], P('groups', None, 'seq'), parts along dimension 0
The draws below stay inside these ranges and needn't reach their ends.
There are 2 independent parts, one for each index of `groups`. The reference program is written for one: setup_inputs(seed, part) draws one part's arguments, and reference() takes and returns one part's arrays. A program takes and returns all parts, laid end to end along the dimension named above; an argument that names none is the same for every part. Nothing has to cross between parts.
Inputs may be any that keep to these rules, and one draw needn't show every extreme that they name: `query_ids`: query ids never fall along the tokens; each of the 3 queries has at least one and at most 128 tokens.
All inputs are finite; a program needn't handle non-finite values.
Results may differ from the reference program's by a relative error of at most 0.006.
Values may be sent and summed in bfloat16 or wider, within the bound.
A program may use at most 128 MiB of HBM per device.

```python
import math
import jax
import jax.numpy as jnp
import numpy as np

D = 2048
FF = 14336
FB = 224
QUERIES = 3
TOKENS = 256
BLOCKS = 64


def level_of(key, dims, shards, least, largest):
    factor_of, own = 1.0, jax.random.fold_in(key, 6)
    for position, shards_of in shards:
        steps = jnp.exp(jax.random.uniform(jax.random.fold_in(own, position), (shards_of,), jnp.float32, least / len(shards), largest / len(shards)))
        factor_of = factor_of * jnp.repeat(steps, dims[position] // shards_of).reshape([-1 if axis == position else 1 for axis in range(len(dims))])
    return factor_of


def profile(count, total, reach, slope):
    weights = [(1 << 20) // math.isqrt(standing ** slope) + 1 for standing in range(2, count + 1)]
    spare, given = total - reach - (count - 1), [1] * (count - 1)
    while spare > 0:
        free = [i for i in range(count - 1) if given[i] < reach]
        mass, remaining = sum([weights[i] for i in free]), spare
        for i in free:
            more = min(reach - given[i], max(1, remaining * weights[i] // mass), spare)
            given[i] = given[i] + more
            spare = spare - more
    return np.array([reach] + given)


def ragged(rng, amount, total, reach, skew):
    if amount == 2:
        one = jax.random.randint(rng, (), max(1, total - reach), min(reach, total - 1) + 1)
        return jnp.stack([one, total - one])
    tallies = jnp.asarray(profile(amount, total, reach, skew), jnp.int32)
    couples = (amount - 1) // 2
    donor, sink = tallies[1:1 + 2 * couples:2], tallies[2:2 + 2 * couples:2]
    room = jnp.minimum(donor - 1, reach - sink)
    passed = jax.random.randint(jax.random.fold_in(rng, 1), (couples,), 0, 1 << 20) % (room + 1)
    tallies = tallies.at[1:1 + 2 * couples:2].set(donor - passed).at[2:2 + 2 * couples:2].set(sink + passed)
    return tallies[jax.random.permutation(jax.random.fold_in(rng, 2), amount)]


def normal_values(rng, extent, spread, most, pieces=(), held_as=jnp.bfloat16):
    gain = level_of(rng, extent, pieces, -0.22, 0.18) if pieces else 1.0
    entries = jax.random.normal(rng, extent, jnp.float32) * spread * gain
    return jnp.minimum(jnp.maximum(entries, -most), most).astype(held_as)


def setup_inputs(seed: int = 0, part: int = 0) -> dict:
    seeds = jax.random.split(jax.random.key(seed), 7)
    part_splits = jax.random.split(jax.random.fold_in(seeds[6], part), 7)
    activations = normal_values(part_splits[0], (TOKENS, FF), 1.0, 6.0, ((0, 16),))
    out_grads = normal_values(part_splits[1], (TOKENS, D), 1.0, 6.0, ((0, 16),))
    query_ids = jnp.searchsorted(jnp.cumsum(ragged(part_splits[2], QUERIES, TOKENS, TOKENS // 2, 0)), jnp.arange(TOKENS), side="right").astype(jnp.int32)
    act_basis = normal_values(seeds[3], (BLOCKS, FB, FB), FB ** -0.5, 0.375, ((0, 16),))
    grad_basis = normal_values(seeds[4], (D, D), D ** -0.5, 0.125, ((1, 16),))
    eigenvalues = jnp.clip(jnp.exp(math.log(80.0) - 2.3025851 * jax.random.uniform(seeds[5], (D, FF), jnp.float32) ** level_of(seeds[5], (D, FF), ((1, 16),), -0.2, 0.2)), 8.0, 80.0)
    return dict(activations=activations, out_grads=out_grads, query_ids=query_ids, act_basis=act_basis, grad_basis=grad_basis, eigenvalues=eigenvalues)


def reference(activations, out_grads, query_ids, act_basis, grad_basis, eigenvalues):
    all_tokens = activations.shape[0]
    blocks = act_basis.shape[0]
    block_order = act_basis.shape[1]
    out_units = grad_basis.shape[0]
    basis_wide = act_basis.astype(jnp.float32)
    rotated_act = jnp.einsum("tbi,bik->tbk", activations.reshape(all_tokens, blocks, block_order).astype(jnp.float32), basis_wide)
    rotated_act = rotated_act.astype(jnp.bfloat16).reshape(all_tokens, blocks * block_order)
    rotated_grad = jnp.dot(out_grads, grad_basis, preferred_element_type=jnp.float32).astype(jnp.bfloat16)
    outputs = []
    for query_index in range(QUERIES):
        selected = jnp.where((query_ids == query_index)[:, None], rotated_act, jnp.zeros_like(rotated_act))
        moments = jnp.dot(rotated_grad.T, selected, preferred_element_type=jnp.float32)
        scaled = (moments / eigenvalues).astype(jnp.bfloat16)
        rotated_back = jnp.einsum("dbk,bik->dbi", scaled.reshape(out_units, blocks, block_order).astype(jnp.float32), basis_wide)
        rotated_back = rotated_back.astype(jnp.bfloat16).reshape(out_units, blocks * block_order)
        outputs.append(jnp.dot(grad_basis, rotated_back, preferred_element_type=jnp.float32).astype(jnp.bfloat16))
    return jnp.stack(outputs, axis=0)
```

```python
import functools

import jax
import jax.numpy as jnp
from jax import lax
from jax.experimental import pallas as pl
from jax.experimental.pallas import tpu as pltpu
from jax.sharding import PartitionSpec as P

QUERIES = 3
LANES = 128
TILE = 256
TALL = 512
STEP = 896


def bands(width, order):
    out = []
    for start in range(0, width, TILE):
        stop = min(start + TILE, width)
        low = start // order * order // LANES * LANES
        high = min(width, -(-(((stop - 1) // order + 1) * order) // LANES) * LANES)
        out.append((start, stop, low, high))
    return out


def back_kernel(order, basis_ref, grads_ref, act_ref, ids_ref, eig_ref, turn_ref, out_ref):
    rotated = jnp.dot(grads_ref[...], basis_ref[...], preferred_element_type=jnp.float32)
    rotated = rotated.astype(jnp.bfloat16)
    act = act_ref[...]
    ids = ids_ref[...]
    for query in range(QUERIES):
        selected = act * (ids == query).astype(jnp.bfloat16)
        moments = lax.dot_general(
            rotated, selected, (((0,), (0,)), ((), ())), preferred_element_type=jnp.float32
        )
        scaled = (moments / eig_ref[...]).astype(jnp.bfloat16)
        for start, stop, low, high in bands(act.shape[1], order):
            out_ref[query, :, start:stop] = jnp.dot(
                scaled[:, low:high], turn_ref[low:high, start:stop], preferred_element_type=jnp.float32
            ).astype(jnp.bfloat16)


def final_kernel(chunks, *refs):
    basis, back, out_ref = refs[:chunks], refs[chunks : 2 * chunks], refs[-1]
    total = None
    for g, b in zip(basis, back):
        term = jnp.dot(g[...], b[0], preferred_element_type=jnp.float32)
        total = term if total is None else total + term
    out_ref[0] = total.astype(jnp.bfloat16)


def ring_shards(groups, n, activations, out_grads, query_ids, act_basis, grad_basis, eigenvalues):
    own_tokens = activations.shape[0]
    blocks, order = act_basis.shape[:2]
    units, cols = grad_basis.shape
    width = blocks * order
    tokens = own_tokens * n
    outer = n // 4
    me, group = lax.axis_index("seq"), lax.axis_index("groups")
    z, y, c = me // 4, me // 2 % 2, me % 2

    ring = [(i, (i + 4) % n) for i in range(n)]
    side = [(i, i ^ 2) for i in range(n)]
    core = [(i, i ^ 1) for i in range(n)]

    pieces = [grad_basis]
    for _ in range(outer - 1):
        pieces.append(lax.ppermute(pieces[-1], "seq", ring))
    chunks, eigs = [], []
    for step, piece in enumerate(pieces):
        if groups == 2 and units % 32 == 0:
            half = units // 2
            sent = lax.dynamic_slice_in_dim(piece, group * half, half, axis=0)
            mine = lax.ppermute(sent, "seq", side)
            theirs = lax.ppermute(mine, "groups", [(0, 1), (1, 0)])
            first = group == 0
            other = jnp.concatenate(
                [jnp.where(first, mine, theirs), jnp.where(first, theirs, mine)], axis=0
            )
        else:
            other = lax.ppermute(piece, "seq", side)
        pair = jnp.concatenate([piece, other], axis=1)
        chunks.append(jnp.concatenate([pair, lax.ppermute(pair, "seq", core)], axis=1))
        level = (z - step) % outer * 4
        origins = [level + yy * 2 + cc for cc in (c, 1 - c) for yy in (y, 1 - y)]
        eigs.append(
            jnp.concatenate(
                [lax.dynamic_slice_in_dim(eigenvalues, o * cols, cols, axis=0) for o in origins], axis=0
            )
        )

    ids = jnp.broadcast_to(query_ids.astype(jnp.bfloat16)[:, None, None], (own_tokens, n, LANES))
    every = jnp.broadcast_to(out_grads[:, None, :], (own_tokens, n, units))
    sent = jnp.concatenate([activations.reshape(own_tokens, n, width), ids, every], axis=2)
    columns = lax.all_to_all(
        jnp.transpose(sent, (1, 0, 2)), "seq", split_axis=0, concat_axis=0, tiled=True
    ).reshape(tokens, width + LANES + units)
    token_query = columns[:, width : width + 1].astype(jnp.float32)
    grads = columns[:, width + LANES :]

    wide = jnp.concatenate(
        [
            jnp.pad(act_basis[b], ((0, 0), (b * order, width - (b + 1) * order)))
            for b in range(blocks)
        ],
        axis=0,
    )
    turned = wide.T
    act = jnp.dot(columns[:, :width], wide, preferred_element_type=jnp.float32).astype(jnp.bfloat16)

    chunk_cols = 4 * cols
    backs = [
        pl.pallas_call(
            functools.partial(back_kernel, order),
            out_shape=jax.ShapeDtypeStruct((QUERIES, chunk_cols, width), jnp.bfloat16),
            in_specs=[pl.BlockSpec(memory_space=pltpu.VMEM)] * 6,
            out_specs=pl.BlockSpec(memory_space=pltpu.VMEM),
            compiler_params=pltpu.CompilerParams(vmem_limit_bytes=40 * 2**20),
            cost_estimate=pl.CostEstimate(
                flops=2 * chunk_cols * (tokens * units + QUERIES * width * (tokens + width // 2)),
                bytes_accessed=2 * units * (chunk_cols + tokens) + 10 * chunk_cols * width,
                transcendentals=0,
            ),
            name="back",
        )(chunk, grads, act, token_query, eig, turned)
        for chunk, eig in zip(chunks, eigs)
    ]

    rows = min(units, 512)
    return pl.pallas_call(
        functools.partial(final_kernel, outer),
        grid=(QUERIES, units // rows),
        out_shape=jax.ShapeDtypeStruct((QUERIES, units, width), jnp.bfloat16),
        in_specs=[pl.BlockSpec((rows, chunk_cols), lambda q, r: (r, 0))] * outer
        + [pl.BlockSpec((1, chunk_cols, width), lambda q, r: (q, 0, 0))] * outer,
        out_specs=pl.BlockSpec((1, rows, width), lambda q, r: (q, r, 0)),
        compiler_params=pltpu.CompilerParams(vmem_limit_bytes=40 * 2**20),
        cost_estimate=pl.CostEstimate(
            flops=2 * QUERIES * units * units * width,
            bytes_accessed=2 * units * units + 4 * QUERIES * units * width,
            transcendentals=0,
        ),
        name="final",
    )(*chunks, *backs)


MESH = pl.DeviceIdType.MESH
LAYERS = 4
PIECES = (0, 432, 864)


class Sends:
    def __init__(self, sems):
        self.sems, self.made = sems, []

    def start(self, src, dst, arrived, device, cond=None):
        def make(i=len(self.made)):
            return pltpu.make_async_remote_copy(
                src_ref=src(), dst_ref=dst(), send_sem=self.sems.at[i], recv_sem=arrived(),
                device_id=device, device_id_type=MESH,
            )

        self.made.append((make, cond))
        if cond is None:
            make().start()
        else:
            pl.when(cond)(lambda: make().start())

    def finish(self):
        for make, cond in self.made:
            if cond is None:
                make().wait_send()
            else:
                pl.when(cond)(lambda make=make: make().wait_send())


def cuts(width):
    return [
        (query, start, min(start + STEP, width)) for query in range(QUERIES) for start in range(0, width, STEP)
    ]


def run(events):
    for event in events:
        event()


def layer_at(step, z):
    table = ((0, 1, 2, 3), (1, 0, 2, 3), (2, 1, 3, 0), (3, 2, 1, 0))
    out = jnp.int32(table[0][step])
    for row in range(1, LAYERS):
        out = jnp.where(z == row, jnp.int32(table[row][step]), out)
    return out


def gather_kernel(
    order, acts_ref, grads_ref, ids_ref, blocks_ref, own_ref, eig_ref,
    out_ref,
    acc_ref, g_ref, gr, ac, idb, ra, wide, turned, eigb, backs, rgt,
    send_sems, local_sems, g_sems, grz_sems, gry_sems, grc_sems, many_sems,
):
    own_tokens = ids_ref.shape[0]
    units, cols = own_ref.shape
    width = ac.shape[1]
    half = units // 2
    edges = [half * e // 1024 // 16 * 16 for e in PIECES] + [half]
    parts = range(len(PIECES))
    count = len(PIECES)
    deep = 4 * cols
    n = 4 * LAYERS
    x, s = lax.axis_index("groups"), lax.axis_index("seq")
    z, y, c = s // 4, s // 2 % 2, s % 2
    layers = [layer_at(t, z) for t in range(LAYERS)]

    def dev(zz, yy, cc):
        return (x, (zz * 2 + yy) * 2 + cc)

    x_mate, y_mate, c_mate = (1 - x, s), dev(z, 1 - y, c), dev(z, y, 1 - c)

    def token_rows(zz, yy, cc, count=1):
        start = ((yy * 2 + cc) * LAYERS + zz) * own_tokens
        return pl.ds(pl.multiple_of(start, own_tokens), count * own_tokens)

    def piece(slot, p):
        side, i = p
        return g_ref.at[slot, pl.ds(pl.multiple_of(side * half + edges[i], 16), edges[i + 1] - edges[i])]

    def slot_of(zz, yy, cc):
        return (zz * 2 + yy) * 2 + cc

    me = slot_of(z, y, c)
    column_slots = [slot_of(layer, y, c) for layer in layers]
    other_slots = [slot_of(layer, 1 - y, c) for layer in layers]
    core_slots = [[slot_of(layer, yy, 1 - c) for yy in (y, 1 - y)] for layer in layers]
    onward = [jnp.where(layer < z, z + 1, z - 1) for layer in layers]
    goes_on = [jnp.logical_and(to >= 0, to < LAYERS) for to in onward]
    beyond = [dev(to, y, c) for to in onward]
    halves = [(x, i) for i in parts]
    mate_halves = [(1 - x, i) for i in parts]
    mine = token_rows(z, y, c)

    local = [
        pltpu.make_async_copy(own_ref, g_ref.at[me], local_sems.at[0]),
        pltpu.make_async_copy(grads_ref, gr.at[mine], local_sems.at[1]),
        pltpu.make_async_copy(acts_ref.at[:, pl.ds(pl.multiple_of(s * width, 128), width)], ac.at[mine], local_sems.at[2]),
        pltpu.make_async_copy(ids_ref, idb.at[mine], local_sems.at[3]),
    ]
    for copy in local:
        copy.start()

    def eig_copy(t):
        at = pl.ds(pl.multiple_of(layers[t] * deep, deep), deep)
        return pltpu.make_async_copy(eig_ref.at[at], eigb.at[t % 2], local_sems.at[4 + t % 2])

    eig_copy(0).start()
    eig_copy(1).start()

    barrier = pltpu.get_barrier_semaphore()
    peers = [(x, lax.rem(s + k, n)) for k in range(1, n)]
    for peer in peers + [x_mate]:
        pl.semaphore_signal(barrier, inc=1, device_id=peer, device_id_type=MESH)
    pl.semaphore_wait(barrier, n)

    sends = Sends(send_sems)

    def send_grads(at, arrived, device):
        sends.start(lambda: gr.at[at], lambda: gr.at[at], arrived, device)

    def send_piece(slot, p, device, cond=None):
        sends.start(lambda: piece(slot, p), lambda: piece(slot, p), lambda: g_sems.at[slot, p[0] * count + p[1]], device, cond)

    def wait_piece(slot, p):
        pltpu.make_async_copy(piece(slot, p), piece(slot, p), g_sems.at[slot, p[0] * count + p[1]]).wait()

    local[1].wait()
    for k in range(1, LAYERS):
        send_grads(mine, lambda: grz_sems.at[z], dev(lax.rem(z + k, LAYERS), y, c))
    send_grads(mine, lambda: gry_sems.at[z], y_mate)
    for peer in peers:
        sends.start(lambda: ids_ref, lambda: idb.at[mine], lambda: many_sems.at[0], peer)
    for peer in peers:
        at = pl.ds(pl.multiple_of(peer[1] * width, 128), width)
        sends.start(lambda at=at: acts_ref.at[:, at], lambda: ac.at[mine], lambda: many_sems.at[1], peer)
    local[0].wait()
    for i in parts:
        send_piece(me, halves[i], y_mate)
        send_piece(me, halves[i], dev(z + 1, y, c), z < LAYERS - 1)
        send_piece(me, halves[i], dev(z - 1, y, c), z > 0)
    for p in halves + mate_halves:
        send_piece(me, p, c_mate)

    wide[...] = jnp.zeros_like(wide)
    turned[...] = jnp.zeros_like(turned)
    for b in range(blocks_ref.shape[0]):
        at = slice(b * order, (b + 1) * order)
        wide[at, at] = blocks_ref[b]
        turned[at, at] = blocks_ref[b].T

    for k in range(1, LAYERS):
        far = lax.rem(z + k, LAYERS)
        at = token_rows(far, y, c)
        pltpu.make_async_copy(gr.at[at], gr.at[at], grz_sems.at[far]).wait()
        send_grads(at, lambda far=far: gry_sems.at[far], y_mate)
    column = token_rows(0, y, c, LAYERS)
    send_grads(column, lambda: grc_sems.at[0], c_mate)
    send_piece(me, mate_halves[-1], y_mate)

    def from_y(t, i):
        slot = other_slots[t]
        wait_piece(slot, halves[i])
        if i < count - 1:
            send_piece(slot, halves[i], x_mate)
        send_piece(slot, halves[i], c_mate)

    def from_z(t, i):
        slot = column_slots[t]
        wait_piece(slot, halves[i])
        send_piece(slot, halves[i], beyond[t], goes_on[t])
        send_piece(slot, halves[i], x_mate)
        send_piece(slot, halves[i], y_mate)
        send_piece(slot, halves[i], c_mate)

    def from_x(t, i):
        slot = column_slots[t]
        wait_piece(slot, mate_halves[i])
        if i == count - 1:
            send_piece(slot, mate_halves[i], y_mate)
        send_piece(slot, mate_halves[i], c_mate)

    def diagonal(t, i):
        slot = other_slots[t]
        wait_piece(slot, mate_halves[i])
        send_piece(slot, mate_halves[i], c_mate)

    def from_core(t):
        for slot in core_slots[t]:
            for p in halves + mate_halves:
                wait_piece(slot, p)

    for i in parts:
        from_y(0, i)
    for k in range(LAYERS):
        far = lax.rem(z + k, LAYERS)
        at = token_rows(far, 1 - y, c)
        pltpu.make_async_copy(gr.at[at], gr.at[at], gry_sems.at[far]).wait()
    other = token_rows(0, 1 - y, c, LAYERS)
    send_grads(other, lambda: grc_sems.at[1], c_mate)
    for i in parts:
        diagonal(0, i)
    for i, yy in enumerate((y, 1 - y)):
        at = token_rows(0, yy, 1 - c, LAYERS)
        pltpu.make_async_copy(gr.at[at], gr.at[at], grc_sems.at[i]).wait()
    from_core(0)

    def rotate_grads(t):
        base = layers[t] * 4
        both = jnp.concatenate([g_ref[base + i] for i in range(4)], axis=1)
        rg = jnp.dot(gr[...], both, preferred_element_type=jnp.float32).astype(jnp.bfloat16)
        rgt[...] = rg.T

    def scale_back(t, out, events):
        eig_copy(t).wait()
        tall = deep // 2

        def body(r, carry):
            at = pl.ds(pl.multiple_of(r * tall, tall), tall)
            inverse = 1.0 / eigb[t % 2, at, :]
            turned_grads = rgt[at, :]
            for query in range(QUERIES):
                moments = jnp.dot(
                    turned_grads, ra[:, query * width : (query + 1) * width], preferred_element_type=jnp.float32
                )
                scaled = (moments * inverse).astype(jnp.bfloat16)
                for start, stop, low, high in bands(width, order):
                    out[at, query * width + start : query * width + stop] = jnp.dot(
                        scaled[:, low:high], turned[low:high, start:stop], preferred_element_type=jnp.float32
                    ).astype(jnp.bfloat16)
            for k, todo in enumerate(events):
                if todo:
                    pl.when(r == k)(functools.partial(run, todo))
            return carry

        lax.fori_loop(0, 2, body, 0)
        if t + 2 < LAYERS:
            eig_copy(t + 2).start()

    def accumulate(t, events):
        base = layers[t] * 4

        def body(r, carry):
            at = pl.ds(pl.multiple_of(r * TALL, TALL), TALL)
            left = jnp.concatenate([g_ref[base + i, at, :] for i in range(4)], axis=1)
            for query, start, stop in cuts(width):
                term = jnp.dot(
                    left, backs[:, query * width + start : query * width + stop], preferred_element_type=jnp.float32
                )
                if t == 0:
                    acc_ref[at, query * width + start : query * width + stop] = term
                elif t < LAYERS - 1:
                    acc_ref[at, query * width + start : query * width + stop] += term
                else:
                    total = acc_ref[at, query * width + start : query * width + stop] + term
                    out_ref[query, at, start:stop] = total.astype(jnp.bfloat16)
            for k, todo in enumerate(events):
                if todo:
                    pl.when(r == k)(functools.partial(run, todo))
            return carry

        lax.fori_loop(0, units // TALL, body, 0)

    def later(f, *args):
        return lambda: f(*args)

    rotate_grads(0)
    local[2].wait()
    local[3].wait()
    others = pl.ds(0, (n - 1) * own_tokens)
    pltpu.make_async_copy(idb.at[others], idb.at[others], many_sems.at[0]).wait()
    pltpu.make_async_copy(ac.at[others], ac.at[others], many_sems.at[1]).wait()
    ids = idb[...].astype(jnp.float32)[:, 0:1]
    for start, stop, low, high in bands(width, order):
        turned_act = jnp.dot(ac[:, low:high], wide[low:high, start:stop], preferred_element_type=jnp.float32)
        turned_act = turned_act.astype(jnp.bfloat16)
        for query in range(QUERIES):
            ra[:, query * width + start : query * width + stop] = turned_act * (ids == query).astype(jnp.bfloat16)

    def all_of(f, t):
        return [later(f, t, i) for i in parts]

    scale_back(0, backs, [all_of(from_z, 1), []])
    accumulate(0, [
        all_of(from_x, 1) + all_of(from_y, 1),
        all_of(from_z, 2),
        all_of(diagonal, 1) + all_of(from_x, 2) + all_of(from_y, 2),
        all_of(from_z, 3) + [later(from_core, 1)],
    ])
    rotate_grads(1)
    scale_back(1, backs, [[], []])
    accumulate(1, [
        all_of(diagonal, 2),
        all_of(from_x, 3),
        all_of(from_y, 3),
        [later(from_core, 2)] + all_of(diagonal, 3),
    ])
    rotate_grads(2)
    scale_back(2, backs, [[], []])
    accumulate(2, [[], [], [], [later(from_core, 3)]])
    rotate_grads(3)
    scale_back(3, backs, [[], []])
    accumulate(3, [])
    sends.finish()


def square_shards(n, activations, out_grads, query_ids, act_basis, grad_basis, eigenvalues):
    own_tokens = activations.shape[0]
    blocks, order = act_basis.shape[:2]
    units, cols = grad_basis.shape
    width = blocks * order
    tokens = own_tokens * n
    deep = 4 * cols
    ids = jnp.broadcast_to(query_ids.astype(jnp.bfloat16)[:, None], (own_tokens, LANES))
    hbm, vmem = pl.BlockSpec(memory_space=pltpu.HBM), pl.BlockSpec(memory_space=pltpu.VMEM)
    return pl.pallas_call(
        functools.partial(gather_kernel, order),
        out_shape=pltpu.VMEM((QUERIES, units, width), jnp.bfloat16),
        in_specs=[hbm, hbm, hbm, vmem, hbm, hbm],
        out_specs=vmem,
        scratch_shapes=[
            pltpu.VMEM((units, QUERIES * width), jnp.float32),
            pltpu.VMEM((n, units, cols), jnp.bfloat16),
            pltpu.VMEM((tokens, units), jnp.bfloat16),
            pltpu.VMEM((tokens, width), jnp.bfloat16),
            pltpu.VMEM((tokens, LANES), jnp.bfloat16),
            pltpu.VMEM((tokens, QUERIES * width), jnp.bfloat16),
            pltpu.VMEM((width, width), jnp.bfloat16),
            pltpu.VMEM((width, width), jnp.bfloat16),
            pltpu.VMEM((2, deep, width), jnp.float32),
            pltpu.VMEM((deep, QUERIES * width), jnp.bfloat16),
            pltpu.VMEM((deep, tokens), jnp.bfloat16),
            pltpu.SemaphoreType.DMA((192,)),
            pltpu.SemaphoreType.DMA((6,)),
            pltpu.SemaphoreType.DMA((n, 2 * len(PIECES))),
            pltpu.SemaphoreType.DMA((LAYERS,)),
            pltpu.SemaphoreType.DMA((LAYERS,)),
            pltpu.SemaphoreType.DMA((2,)),
            pltpu.SemaphoreType.DMA((2,)),
        ],
        compiler_params=pltpu.CompilerParams(
            collective_id=0, has_side_effects=True, vmem_limit_bytes=50 * 2**20
        ),
        cost_estimate=pl.CostEstimate(
            flops=2 * QUERIES * units * units * width, bytes_accessed=4 * units * width, transcendentals=0
        ),
        name="gather",
    )(activations, out_grads, ids, act_basis, grad_basis, eigenvalues)


def shards(groups, n, activations, out_grads, query_ids, act_basis, grad_basis, eigenvalues):
    args = activations, out_grads, query_ids, act_basis, grad_basis, eigenvalues
    units, cols = grad_basis.shape
    width = act_basis.shape[0] * act_basis.shape[1]
    if groups == 2 and n == 4 * LAYERS and cols % LANES == 0 and width % LANES == 0 and units % 1024 == 0:
        return square_shards(n, *args)
    return ring_shards(groups, n, *args)


def solution(mesh):
    return jax.shard_map(
        functools.partial(shards, mesh.shape["groups"], mesh.shape["seq"]),
        mesh=mesh,
        in_specs=(
            P(("groups", "seq"), None),
            P(("groups", "seq"), None),
            P(("groups", "seq")),
            P("seq", None, None),
            P(None, "seq"),
            P(None, "seq"),
        ),
        out_specs=P("groups", None, "seq"),
        check_vma=False,
    )
```

```python
import functools

import jax
import jax.numpy as jnp
from jax import lax
from jax.experimental import pallas as pl
from jax.experimental.pallas import tpu as pltpu
from jax.sharding import PartitionSpec as P

QUERIES = 3
LANES = 128
TILE = 256
TALL = 512
STEP = 768


def bands(width, order):
    out = []
    for start in range(0, width, TILE):
        stop = min(start + TILE, width)
        low = start // order * order // LANES * LANES
        high = min(width, -(-(((stop - 1) // order + 1) * order) // LANES) * LANES)
        out.append((start, stop, low, high))
    return out


def back_kernel(order, basis_ref, grads_ref, act_ref, ids_ref, eig_ref, turn_ref, out_ref):
    rotated = jnp.dot(grads_ref[...], basis_ref[...], preferred_element_type=jnp.float32)
    rotated = rotated.astype(jnp.bfloat16)
    act = act_ref[...]
    ids = ids_ref[...]
    for query in range(QUERIES):
        selected = act * (ids == query).astype(jnp.bfloat16)
        moments = lax.dot_general(
            rotated, selected, (((0,), (0,)), ((), ())), preferred_element_type=jnp.float32
        )
        scaled = (moments / eig_ref[...]).astype(jnp.bfloat16)
        for start, stop, low, high in bands(act.shape[1], order):
            out_ref[query, :, start:stop] = jnp.dot(
                scaled[:, low:high], turn_ref[low:high, start:stop], preferred_element_type=jnp.float32
            ).astype(jnp.bfloat16)


def final_kernel(chunks, *refs):
    basis, back, out_ref = refs[:chunks], refs[chunks : 2 * chunks], refs[-1]
    total = None
    for g, b in zip(basis, back):
        term = jnp.dot(g[...], b[0], preferred_element_type=jnp.float32)
        total = term if total is None else total + term
    out_ref[0] = total.astype(jnp.bfloat16)


def ring_shards(groups, n, activations, out_grads, query_ids, act_basis, grad_basis, eigenvalues):
    own_tokens = activations.shape[0]
    blocks, order = act_basis.shape[:2]
    units, cols = grad_basis.shape
    width = blocks * order
    tokens = own_tokens * n
    outer = n // 4
    me, group = lax.axis_index("seq"), lax.axis_index("groups")
    z, y, c = me // 4, me // 2 % 2, me % 2

    ring = [(i, (i + 4) % n) for i in range(n)]
    side = [(i, i ^ 2) for i in range(n)]
    core = [(i, i ^ 1) for i in range(n)]

    pieces = [grad_basis]
    for _ in range(outer - 1):
        pieces.append(lax.ppermute(pieces[-1], "seq", ring))
    chunks, eigs = [], []
    for step, piece in enumerate(pieces):
        if groups == 2 and units % 32 == 0:
            half = units // 2
            sent = lax.dynamic_slice_in_dim(piece, group * half, half, axis=0)
            mine = lax.ppermute(sent, "seq", side)
            theirs = lax.ppermute(mine, "groups", [(0, 1), (1, 0)])
            first = group == 0
            other = jnp.concatenate(
                [jnp.where(first, mine, theirs), jnp.where(first, theirs, mine)], axis=0
            )
        else:
            other = lax.ppermute(piece, "seq", side)
        pair = jnp.concatenate([piece, other], axis=1)
        chunks.append(jnp.concatenate([pair, lax.ppermute(pair, "seq", core)], axis=1))
        level = (z - step) % outer * 4
        origins = [level + yy * 2 + cc for cc in (c, 1 - c) for yy in (y, 1 - y)]
        eigs.append(
            jnp.concatenate(
                [lax.dynamic_slice_in_dim(eigenvalues, o * cols, cols, axis=0) for o in origins], axis=0
            )
        )

    ids = jnp.broadcast_to(query_ids.astype(jnp.bfloat16)[:, None, None], (own_tokens, n, LANES))
    every = jnp.broadcast_to(out_grads[:, None, :], (own_tokens, n, units))
    sent = jnp.concatenate([activations.reshape(own_tokens, n, width), ids, every], axis=2)
    columns = lax.all_to_all(
        jnp.transpose(sent, (1, 0, 2)), "seq", split_axis=0, concat_axis=0, tiled=True
    ).reshape(tokens, width + LANES + units)
    token_query = columns[:, width : width + 1].astype(jnp.float32)
    grads = columns[:, width + LANES :]

    wide = jnp.concatenate(
        [
            jnp.pad(act_basis[b], ((0, 0), (b * order, width - (b + 1) * order)))
            for b in range(blocks)
        ],
        axis=0,
    )
    turned = wide.T
    act = jnp.dot(columns[:, :width], wide, preferred_element_type=jnp.float32).astype(jnp.bfloat16)

    chunk_cols = 4 * cols
    backs = [
        pl.pallas_call(
            functools.partial(back_kernel, order),
            out_shape=jax.ShapeDtypeStruct((QUERIES, chunk_cols, width), jnp.bfloat16),
            in_specs=[pl.BlockSpec(memory_space=pltpu.VMEM)] * 6,
            out_specs=pl.BlockSpec(memory_space=pltpu.VMEM),
            compiler_params=pltpu.CompilerParams(vmem_limit_bytes=40 * 2**20),
            cost_estimate=pl.CostEstimate(
                flops=2 * chunk_cols * (tokens * units + QUERIES * width * (tokens + width // 2)),
                bytes_accessed=2 * units * (chunk_cols + tokens) + 10 * chunk_cols * width,
                transcendentals=0,
            ),
            name="back",
        )(chunk, grads, act, token_query, eig, turned)
        for chunk, eig in zip(chunks, eigs)
    ]

    rows = min(units, 512)
    return pl.pallas_call(
        functools.partial(final_kernel, outer),
        grid=(QUERIES, units // rows),
        out_shape=jax.ShapeDtypeStruct((QUERIES, units, width), jnp.bfloat16),
        in_specs=[pl.BlockSpec((rows, chunk_cols), lambda q, r: (r, 0))] * outer
        + [pl.BlockSpec((1, chunk_cols, width), lambda q, r: (q, 0, 0))] * outer,
        out_specs=pl.BlockSpec((1, rows, width), lambda q, r: (q, r, 0)),
        compiler_params=pltpu.CompilerParams(vmem_limit_bytes=40 * 2**20),
        cost_estimate=pl.CostEstimate(
            flops=2 * QUERIES * units * units * width,
            bytes_accessed=2 * units * units + 4 * QUERIES * units * width,
            transcendentals=0,
        ),
        name="final",
    )(*chunks, *backs)


MESH = pl.DeviceIdType.MESH
LAYERS = 4
PIECES = (0, 256, 512, 768)
EVENTS = (
    (
        (),
        (
            ("g", 1, 0), ("g", 3, 0), ("g", 2, 0), ("y", 0, 0), ("y", 0, 1), ("y", 0, 2), ("d", 0, 0), ("y", 0, 3),
            ("d", 0, 1), ("z", 1, 0), ("d", 0, 2), ("z", 1, 1), ("z", 1, 2), ("h", 0, 0), ("x", 1, 0), ("z", 1, 3),
            ("d", 0, 3), ("x", 1, 1), ("y", 1, 0),
        ),
        (
            ("x", 1, 2),
        ),
        (
            ("y", 1, 1), ("z", 2, 0), ("x", 1, 3),
        ),
        (
            ("y", 1, 2), ("z", 2, 1), ("d", 1, 0), ("y", 1, 3),
        ),
        (
            ("z", 2, 2), ("d", 1, 1), ("y", 2, 0),
        ),
        (
            ("z", 2, 3), ("x", 2, 0), ("d", 1, 3),
        ),
        (
            ("d", 1, 2), ("y", 2, 1), ("z", 3, 0),
        ),
        (
            ("x", 2, 1), ("y", 2, 2), ("z", 3, 1),
        ),
        (
            ("x", 2, 2), ("z", 3, 2), ("y", 2, 3),
        ),
        (
            ("d", 2, 0), ("z", 3, 3), ("y", 3, 0), ("x", 2, 3), ("y", 3, 1),
        ),
        (
            ("d", 2, 1), ("y", 3, 2),
        ),
        (
            ("x", 3, 0), ("d", 2, 2),
        ),
        (
            ("y", 3, 3), ("x", 3, 1),
        ),
        (
            ("d", 2, 3), ("x", 3, 2), ("x", 3, 3),
        ),
        (
            ("d", 3, 0),
        ),
        (
            ("d", 3, 1), ("d", 3, 3),
        ),
        (
            ("d", 3, 2),
        ),
        (),
        (),
        (),
        (),
        (),
        (),
        (),
        (),
        (),
    ),
    (
        (),
        (
            ("g", 1, 0), ("g", 3, 0), ("g", 2, 0), ("y", 0, 0), ("y", 0, 1), ("y", 0, 2), ("d", 0, 0), ("y", 0, 3),
            ("d", 0, 1), ("z", 1, 0), ("d", 0, 2), ("z", 1, 1), ("z", 1, 2), ("h", 0, 0), ("x", 1, 0), ("z", 2, 0),
            ("z", 1, 3), ("d", 0, 3), ("x", 1, 1), ("z", 2, 1), ("y", 1, 0),
        ),
        (
            ("x", 1, 2), ("z", 2, 2), ("y", 1, 1),
        ),
        (
            ("x", 2, 0), ("z", 2, 3),
        ),
        (
            ("y", 1, 2), ("x", 1, 3), ("z", 3, 0), ("y", 2, 0), ("x", 2, 1), ("z", 3, 1),
        ),
        (
            ("y", 1, 3), ("d", 1, 0), ("z", 3, 2),
        ),
        (
            ("y", 2, 1), ("x", 2, 2), ("z", 3, 3),
        ),
        (
            ("y", 2, 2), ("d", 1, 1), ("y", 2, 3),
        ),
        (
            ("x", 2, 3), ("d", 1, 3), ("d", 1, 2), ("y", 3, 0), ("x", 3, 0),
        ),
        (
            ("y", 3, 1), ("d", 2, 0),
        ),
        (
            ("y", 3, 2), ("x", 3, 1), ("y", 3, 3),
        ),
        (
            ("x", 3, 2), ("d", 2, 3), ("d", 2, 1),
        ),
        (
            ("x", 3, 3),
        ),
        (
            ("d", 2, 2),
        ),
        (
            ("d", 3, 0),
        ),
        (
            ("d", 3, 3), ("d", 3, 1),
        ),
        (
            ("d", 3, 2),
        ),
        (),
        (),
        (),
        (),
        (),
        (),
        (),
        (),
        (),
        (),
    ),
)


class Sends:
    def __init__(self, sems):
        self.sems, self.made = sems, {}

    def start(self, key, src, dst, arrived, device, cond=None):
        if key not in self.made:
            index = len(self.made)

            def make():
                return pltpu.make_async_remote_copy(
                    src_ref=src(), dst_ref=dst(), send_sem=self.sems.at[index], recv_sem=arrived(),
                    device_id=device, device_id_type=MESH,
                )

            self.made[key] = make, cond
        make, cond = self.made[key]
        if cond is None:
            make().start()
        else:
            pl.when(cond)(lambda: make().start())

    def finish(self):
        for make, cond in self.made.values():
            if cond is None:
                make().wait_send()
            else:
                pl.when(cond)(lambda make=make: make().wait_send())


def cuts(width):
    return [(start, min(start + STEP, QUERIES * width)) for start in range(0, QUERIES * width, STEP)]


def layer_at(step, z):
    table = ((0, 1, 2, 3), (1, 0, 2, 3), (2, 3, 1, 0), (3, 2, 1, 0))
    out = jnp.int32(table[0][step])
    for row in range(1, LAYERS):
        out = jnp.where(z == row, jnp.int32(table[row][step]), out)
    return out


def gather_kernel(
    order, acts_ref, grads_ref, ids_ref, blocks_ref, own_ref, eig_ref,
    out_ref,
    acc_ref, g_ref, gr, ac, idb, ra, wide, turned, eigb, scaled, backs, rgt,
    send_sems, local_sems, g_sems, grz_sems, gry_sems, grc_sems, many_sems,
):
    own_tokens = ids_ref.shape[0]
    units, cols = own_ref.shape
    width = ac.shape[1]
    half = units // 2
    edges = [half * e // 1024 // 16 * 16 for e in PIECES] + [half]
    parts = range(len(PIECES))
    count = len(PIECES)
    deep = 4 * cols
    n = 4 * LAYERS
    x, s = lax.axis_index("groups"), lax.axis_index("seq")
    z, y, c = s // 4, s // 2 % 2, s % 2
    layers = [layer_at(t, z) for t in range(LAYERS)]

    def dev(zz, yy, cc):
        return (x, (zz * 2 + yy) * 2 + cc)

    x_mate, y_mate, c_mate = (1 - x, s), dev(z, 1 - y, c), dev(z, y, 1 - c)

    def token_rows(zz, yy, cc, count=1):
        start = ((yy * 2 + cc) * LAYERS + zz) * own_tokens
        return pl.ds(pl.multiple_of(start, own_tokens), count * own_tokens)

    def piece(slot, p):
        side, i = p
        return g_ref.at[slot, pl.ds(pl.multiple_of(side * half + edges[i], 16), edges[i + 1] - edges[i])]

    def slot_of(zz, yy, cc):
        return (zz * 2 + yy) * 2 + cc

    me = slot_of(z, y, c)
    column_slots = [slot_of(layer, y, c) for layer in layers]
    other_slots = [slot_of(layer, 1 - y, c) for layer in layers]
    core_slots = [[slot_of(layer, yy, 1 - c) for yy in (y, 1 - y)] for layer in layers]
    onward = [jnp.where(layer < z, z + 1, z - 1) for layer in layers]
    goes_on = [jnp.logical_and(to >= 0, to < LAYERS) for to in onward]
    beyond = [dev(to, y, c) for to in onward]
    halves = [(x, i) for i in parts]
    mate_halves = [(1 - x, i) for i in parts]
    mine = token_rows(z, y, c)

    local = [
        pltpu.make_async_copy(own_ref, g_ref.at[me], local_sems.at[0]),
        pltpu.make_async_copy(grads_ref, gr.at[mine], local_sems.at[1]),
        pltpu.make_async_copy(acts_ref.at[:, pl.ds(pl.multiple_of(s * width, 128), width)], ac.at[mine], local_sems.at[2]),
        pltpu.make_async_copy(ids_ref, idb.at[mine], local_sems.at[3]),
    ]
    for copy in local:
        copy.start()

    def eig_copy(t):
        at = pl.ds(pl.multiple_of(layers[t] * deep, deep), deep)
        return pltpu.make_async_copy(eig_ref.at[at], eigb.at[t % 2], local_sems.at[4 + t % 2])

    eig_copy(0).start()
    eig_copy(1).start()

    barrier = pltpu.get_barrier_semaphore()
    peers = [(x, lax.rem(s + k, n)) for k in range(1, n)]
    for peer in peers + [x_mate]:
        pl.semaphore_signal(barrier, inc=1, device_id=peer, device_id_type=MESH)
    pl.semaphore_wait(barrier, n)

    sends = Sends(send_sems)

    def send_grads(key, at, arrived, device):
        sends.start(("grads", *key), lambda: gr.at[at], lambda: gr.at[at], arrived, device)

    def send_piece(to, key, slot, p, device, cond=None):
        sends.start(
            (to, *key), lambda: piece(slot, p), lambda: piece(slot, p),
            lambda: g_sems.at[slot, p[0] * count + p[1]], device, cond,
        )

    def wait_piece(slot, p):
        pltpu.make_async_copy(piece(slot, p), piece(slot, p), g_sems.at[slot, p[0] * count + p[1]]).wait()

    local[1].wait()
    for t in range(1, LAYERS):
        send_grads(("z", t), mine, lambda: grz_sems.at[z], dev(layers[t], y, c))
    send_grads(("y", 0), mine, lambda: gry_sems.at[z], y_mate)
    for k, peer in enumerate(peers):
        sends.start(("ids", k), lambda: ids_ref, lambda: idb.at[mine], lambda: many_sems.at[0], peer)
    for k, peer in enumerate(peers):
        at = pl.ds(pl.multiple_of(peer[1] * width, 128), width)
        sends.start(("acts", k), lambda at=at: acts_ref.at[:, at], lambda: ac.at[mine], lambda: many_sems.at[1], peer)
    local[0].wait()
    for i in parts:
        send_piece("y", (0, i), me, halves[i], y_mate)
        send_piece("up", (0, i), me, halves[i], dev(z + 1, y, c), z < LAYERS - 1)
        send_piece("down", (0, i), me, halves[i], dev(z - 1, y, c), z > 0)
    for i in parts:
        send_piece("core", ("z", 0, i), me, halves[i], c_mate)
        send_piece("core", ("x", 0, i), me, mate_halves[i], c_mate)

    def from_y(t, i):
        wait_piece(other_slots[t], halves[i])
        if i < count - 1:
            send_piece("x", ("y", t, i), other_slots[t], halves[i], x_mate)
        send_piece("core", ("y", t, i), other_slots[t], halves[i], c_mate)

    def from_z(t, i):
        wait_piece(column_slots[t], halves[i])
        send_piece("on", (t, i), column_slots[t], halves[i], beyond[t], goes_on[t])
        send_piece("x", ("z", t, i), column_slots[t], halves[i], x_mate)
        send_piece("y", (t, i), column_slots[t], halves[i], y_mate)
        send_piece("core", ("z", t, i), column_slots[t], halves[i], c_mate)

    def from_x(t, i):
        wait_piece(column_slots[t], mate_halves[i])
        if i == count - 1:
            send_piece("y", ("x", t, i), column_slots[t], mate_halves[i], y_mate)
        send_piece("core", ("x", t, i), column_slots[t], mate_halves[i], c_mate)

    def diagonal(t, i):
        wait_piece(other_slots[t], mate_halves[i])
        send_piece("core", ("d", t, i), other_slots[t], mate_halves[i], c_mate)

    def from_core(t):
        for slot in core_slots[t]:
            for p in halves + mate_halves:
                wait_piece(slot, p)

    def wait_grads(at, sem):
        pltpu.make_async_copy(gr.at[at], gr.at[at], sem).wait()

    own_rows = [token_rows(layer, y, c) for layer in layers]
    column, other = token_rows(0, y, c, LAYERS), token_rows(0, 1 - y, c, LAYERS)

    def grads_along(t, last):
        wait_grads(own_rows[t], grz_sems.at[layers[t]])
        send_grads(("y", t), own_rows[t], lambda: gry_sems.at[layers[t]], y_mate)
        if last:
            send_grads(("core", 0), column, lambda: grc_sems.at[0], c_mate)
            send_piece("y", ("x", 0, count - 1), me, mate_halves[-1], y_mate)

    def grads_across():
        for layer in range(LAYERS):
            wait_grads(token_rows(layer, 1 - y, c), gry_sems.at[layer])
        send_grads(("core", 1), other, lambda: grc_sems.at[1], c_mate)

    doers = {"x": from_x, "y": from_y, "z": from_z, "d": diagonal}
    at_end = jnp.logical_or(z == 0, z == LAYERS - 1)

    def pass_on(now):
        for place, here in enumerate((at_end, jnp.logical_not(at_end))):
            table = EVENTS[place]
            along = [event for todo in table for event in todo if event[0] == "g"]

            def body(todo=table[now], along=along):
                for kind, t, i in todo:
                    if kind == "g":
                        grads_along(t, (kind, t, i) == along[-1])
                    elif kind == "h":
                        grads_across()
                    else:
                        doers[kind](t, i)

            if table[now]:
                pl.when(here)(body)

    pass_on(0)
    wide[...] = jnp.zeros_like(wide)
    turned[...] = jnp.zeros_like(turned)
    for b in range(blocks_ref.shape[0]):
        at = slice(b * order, (b + 1) * order)
        wide[at, at] = blocks_ref[b]
        turned[at, at] = blocks_ref[b].T

    pass_on(1)
    for i, yy in enumerate((y, 1 - y)):
        wait_grads(token_rows(0, yy, 1 - c, LAYERS), grc_sems.at[i])
    from_core(0)

    def rotate_grads(t):
        base = layers[t] * 4
        both = jnp.concatenate([g_ref[base + i] for i in range(4)], axis=1)
        rg = jnp.dot(gr[...], both, preferred_element_type=jnp.float32).astype(jnp.bfloat16)
        rgt[...] = rg.T

    def scale_back(t):
        eig_copy(t).wait()
        for start, stop in cuts(width):
            moments = jnp.dot(rgt[...], ra[:, start:stop], preferred_element_type=jnp.float32)
            for lane in range(start, stop, LANES):
                value = moments[:, lane - start : lane - start + LANES]
                under = eigb[t % 2, :, lane % width : lane % width + LANES]
                scaled[:, lane : lane + LANES] = (value * (1.0 / under)).astype(jnp.bfloat16)
        for query in range(QUERIES):
            for start, stop, low, high in bands(width, order):
                backs[:, query * width + start : query * width + stop] = jnp.dot(
                    scaled[:, query * width + low : query * width + high], turned[low:high, start:stop],
                    preferred_element_type=jnp.float32,
                ).astype(jnp.bfloat16)
        if t + 2 < LAYERS:
            eig_copy(t + 2).start()

    def accumulate(t, first):
        base = layers[t] * 4

        def body(r, carry):
            at = pl.ds(pl.multiple_of(r * TALL, TALL), TALL)
            left = jnp.concatenate([g_ref[base + i, at, :] for i in range(4)], axis=1)
            for start, stop in cuts(width):
                term = jnp.dot(left, backs[:, start:stop], preferred_element_type=jnp.float32)
                if t > 0:
                    term = acc_ref[at, start:stop] + term
                if t < LAYERS - 1:
                    acc_ref[at, start:stop] = term
                else:
                    for query in range(start // width, (stop - 1) // width + 1):
                        low, high = max(start, query * width), min(stop, (query + 1) * width)
                        out_ref[query, at, low - query * width : high - query * width] = term[
                            :, low - start : high - start
                        ].astype(jnp.bfloat16)
            for k in range(units // TALL):
                if any(table[first + k] for table in EVENTS):
                    pl.when(r == k)(functools.partial(pass_on, first + k))
            return carry

        lax.fori_loop(0, units // TALL, body, 0)

    rotate_grads(0)
    pass_on(2)
    local[2].wait()
    local[3].wait()
    others = pl.ds(0, (n - 1) * own_tokens)
    pltpu.make_async_copy(idb.at[others], idb.at[others], many_sems.at[0]).wait()
    pltpu.make_async_copy(ac.at[others], ac.at[others], many_sems.at[1]).wait()
    ids = idb[...].astype(jnp.float32)[:, 0:1]
    for start, stop, low, high in bands(width, order):
        turned_act = jnp.dot(ac[:, low:high], wide[low:high, start:stop], preferred_element_type=jnp.float32)
        turned_act = turned_act.astype(jnp.bfloat16)
        for query in range(QUERIES):
            ra[:, query * width + start : query * width + stop] = turned_act * (ids == query).astype(jnp.bfloat16)

    pass_on(3)
    now = 4
    for t in range(LAYERS):
        if t > 0:
            from_core(t)
            rotate_grads(t)
            pass_on(now)
            now += 1
        scale_back(t)
        pass_on(now)
        accumulate(t, now + 1)
        now += 1 + units // TALL
    sends.finish()


def square_shards(n, activations, out_grads, query_ids, act_basis, grad_basis, eigenvalues):
    own_tokens = activations.shape[0]
    blocks, order = act_basis.shape[:2]
    units, cols = grad_basis.shape
    width = blocks * order
    tokens = own_tokens * n
    deep = 4 * cols
    ids = jnp.broadcast_to(query_ids.astype(jnp.bfloat16)[:, None], (own_tokens, LANES))
    hbm, vmem = pl.BlockSpec(memory_space=pltpu.HBM), pl.BlockSpec(memory_space=pltpu.VMEM)
    return pl.pallas_call(
        functools.partial(gather_kernel, order),
        out_shape=pltpu.VMEM((QUERIES, units, width), jnp.bfloat16),
        in_specs=[hbm, hbm, hbm, vmem, hbm, hbm],
        out_specs=vmem,
        scratch_shapes=[
            pltpu.VMEM((units, QUERIES * width), jnp.float32),
            pltpu.VMEM((n, units, cols), jnp.bfloat16),
            pltpu.VMEM((tokens, units), jnp.bfloat16),
            pltpu.VMEM((tokens, width), jnp.bfloat16),
            pltpu.VMEM((tokens, LANES), jnp.bfloat16),
            pltpu.VMEM((tokens, QUERIES * width), jnp.bfloat16),
            pltpu.VMEM((width, width), jnp.bfloat16),
            pltpu.VMEM((width, width), jnp.bfloat16),
            pltpu.VMEM((2, deep, width), jnp.float32),
            pltpu.VMEM((deep, QUERIES * width), jnp.bfloat16),
            pltpu.VMEM((deep, QUERIES * width), jnp.bfloat16),
            pltpu.VMEM((deep, tokens), jnp.bfloat16),
            pltpu.SemaphoreType.DMA((240,)),
            pltpu.SemaphoreType.DMA((6,)),
            pltpu.SemaphoreType.DMA((n, 2 * len(PIECES))),
            pltpu.SemaphoreType.DMA((LAYERS,)),
            pltpu.SemaphoreType.DMA((LAYERS,)),
            pltpu.SemaphoreType.DMA((2,)),
            pltpu.SemaphoreType.DMA((2,)),
        ],
        compiler_params=pltpu.CompilerParams(
            collective_id=0, has_side_effects=True, vmem_limit_bytes=51 * 2**20
        ),
        cost_estimate=pl.CostEstimate(
            flops=2 * QUERIES * units * units * width, bytes_accessed=4 * units * width, transcendentals=0
        ),
        name="gather",
    )(activations, out_grads, ids, act_basis, grad_basis, eigenvalues)


def shards(groups, n, activations, out_grads, query_ids, act_basis, grad_basis, eigenvalues):
    args = activations, out_grads, query_ids, act_basis, grad_basis, eigenvalues
    units, cols = grad_basis.shape
    width = act_basis.shape[0] * act_basis.shape[1]
    if groups == 2 and n == 4 * LAYERS and cols % LANES == 0 and width % LANES == 0 and units == 4 * TALL:
        return square_shards(n, *args)
    return ring_shards(groups, n, *args)


def solution(mesh):
    return jax.shard_map(
        functools.partial(shards, mesh.shape["groups"], mesh.shape["seq"]),
        mesh=mesh,
        in_specs=(
            P(("groups", "seq"), None),
            P(("groups", "seq"), None),
            P(("groups", "seq")),
            P("seq", None, None),
            P(None, "seq"),
            P(None, "seq"),
        ),
        out_specs=P("groups", None, "seq"),
        check_vma=False,
    )
```

```python
import functools

import jax
import jax.numpy as jnp
from jax import lax
from jax.experimental import pallas as pl
from jax.experimental.pallas import tpu as pltpu
from jax.sharding import PartitionSpec as P

QUERIES = 3
LANES = 128
TILE = 256
TALL = 512
STEP = 768


def bands(width, order):
    out = []
    for start in range(0, width, TILE):
        stop = min(start + TILE, width)
        low = start // order * order // LANES * LANES
        high = min(width, -(-(((stop - 1) // order + 1) * order) // LANES) * LANES)
        out.append((start, stop, low, high))
    return out


def back_kernel(order, basis_ref, grads_ref, act_ref, ids_ref, eig_ref, turn_ref, out_ref):
    rotated = jnp.dot(grads_ref[...], basis_ref[...], preferred_element_type=jnp.float32)
    rotated = rotated.astype(jnp.bfloat16)
    act = act_ref[...]
    ids = ids_ref[...]
    for query in range(QUERIES):
        selected = act * (ids == query).astype(jnp.bfloat16)
        moments = lax.dot_general(
            rotated, selected, (((0,), (0,)), ((), ())), preferred_element_type=jnp.float32
        )
        scaled = (moments / eig_ref[...]).astype(jnp.bfloat16)
        for start, stop, low, high in bands(act.shape[1], order):
            out_ref[query, :, start:stop] = jnp.dot(
                scaled[:, low:high], turn_ref[low:high, start:stop], preferred_element_type=jnp.float32
            ).astype(jnp.bfloat16)


def final_kernel(chunks, *refs):
    basis, back, out_ref = refs[:chunks], refs[chunks : 2 * chunks], refs[-1]
    total = None
    for g, b in zip(basis, back):
        term = jnp.dot(g[...], b[0], preferred_element_type=jnp.float32)
        total = term if total is None else total + term
    out_ref[0] = total.astype(jnp.bfloat16)


def ring_shards(groups, n, activations, out_grads, query_ids, act_basis, grad_basis, eigenvalues):
    own_tokens = activations.shape[0]
    blocks, order = act_basis.shape[:2]
    units, cols = grad_basis.shape
    width = blocks * order
    tokens = own_tokens * n
    outer = n // 4
    me, group = lax.axis_index("seq"), lax.axis_index("groups")
    z, y, c = me // 4, me // 2 % 2, me % 2

    ring = [(i, (i + 4) % n) for i in range(n)]
    side = [(i, i ^ 2) for i in range(n)]
    core = [(i, i ^ 1) for i in range(n)]

    pieces = [grad_basis]
    for _ in range(outer - 1):
        pieces.append(lax.ppermute(pieces[-1], "seq", ring))
    chunks, eigs = [], []
    for step, piece in enumerate(pieces):
        if groups == 2 and units % 32 == 0:
            half = units // 2
            sent = lax.dynamic_slice_in_dim(piece, group * half, half, axis=0)
            mine = lax.ppermute(sent, "seq", side)
            theirs = lax.ppermute(mine, "groups", [(0, 1), (1, 0)])
            first = group == 0
            other = jnp.concatenate(
                [jnp.where(first, mine, theirs), jnp.where(first, theirs, mine)], axis=0
            )
        else:
            other = lax.ppermute(piece, "seq", side)
        pair = jnp.concatenate([piece, other], axis=1)
        chunks.append(jnp.concatenate([pair, lax.ppermute(pair, "seq", core)], axis=1))
        level = (z - step) % outer * 4
        origins = [level + yy * 2 + cc for cc in (c, 1 - c) for yy in (y, 1 - y)]
        eigs.append(
            jnp.concatenate(
                [lax.dynamic_slice_in_dim(eigenvalues, o * cols, cols, axis=0) for o in origins], axis=0
            )
        )

    ids = jnp.broadcast_to(query_ids.astype(jnp.bfloat16)[:, None, None], (own_tokens, n, LANES))
    every = jnp.broadcast_to(out_grads[:, None, :], (own_tokens, n, units))
    sent = jnp.concatenate([activations.reshape(own_tokens, n, width), ids, every], axis=2)
    columns = lax.all_to_all(
        jnp.transpose(sent, (1, 0, 2)), "seq", split_axis=0, concat_axis=0, tiled=True
    ).reshape(tokens, width + LANES + units)
    token_query = columns[:, width : width + 1].astype(jnp.float32)
    grads = columns[:, width + LANES :]

    wide = jnp.concatenate(
        [
            jnp.pad(act_basis[b], ((0, 0), (b * order, width - (b + 1) * order)))
            for b in range(blocks)
        ],
        axis=0,
    )
    turned = wide.T
    act = jnp.dot(columns[:, :width], wide, preferred_element_type=jnp.float32).astype(jnp.bfloat16)

    chunk_cols = 4 * cols
    backs = [
        pl.pallas_call(
            functools.partial(back_kernel, order),
            out_shape=jax.ShapeDtypeStruct((QUERIES, chunk_cols, width), jnp.bfloat16),
            in_specs=[pl.BlockSpec(memory_space=pltpu.VMEM)] * 6,
            out_specs=pl.BlockSpec(memory_space=pltpu.VMEM),
            compiler_params=pltpu.CompilerParams(vmem_limit_bytes=40 * 2**20),
            cost_estimate=pl.CostEstimate(
                flops=2 * chunk_cols * (tokens * units + QUERIES * width * (tokens + width // 2)),
                bytes_accessed=2 * units * (chunk_cols + tokens) + 10 * chunk_cols * width,
                transcendentals=0,
            ),
            name="back",
        )(chunk, grads, act, token_query, eig, turned)
        for chunk, eig in zip(chunks, eigs)
    ]

    rows = min(units, 512)
    return pl.pallas_call(
        functools.partial(final_kernel, outer),
        grid=(QUERIES, units // rows),
        out_shape=jax.ShapeDtypeStruct((QUERIES, units, width), jnp.bfloat16),
        in_specs=[pl.BlockSpec((rows, chunk_cols), lambda q, r: (r, 0))] * outer
        + [pl.BlockSpec((1, chunk_cols, width), lambda q, r: (q, 0, 0))] * outer,
        out_specs=pl.BlockSpec((1, rows, width), lambda q, r: (q, r, 0)),
        compiler_params=pltpu.CompilerParams(vmem_limit_bytes=40 * 2**20),
        cost_estimate=pl.CostEstimate(
            flops=2 * QUERIES * units * units * width,
            bytes_accessed=2 * units * units + 4 * QUERIES * units * width,
            transcendentals=0,
        ),
        name="final",
    )(*chunks, *backs)


MESH = pl.DeviceIdType.MESH
LAYERS = 4
PIECES = (0, 256, 512, 704, 864)
ACROSS = 2
EVENTS = (
    (
        (),
        (
            ("g", 1, 0), ("g", 3, 0), ("g", 2, 0), ("y", 0, 0), ("y", 0, 1), ("y", 0, 2), ("y", 0, 3), ("d", 0, 0),
            ("y", 0, 4), ("d", 0, 1), ("z", 1, 0), ("d", 0, 2), ("z", 1, 1), ("z", 1, 2), ("h", 0, 0), ("z", 1, 3),
            ("x", 1, 0), ("d", 0, 3), ("z", 1, 4),
        ),
        (
            ("d", 0, 4), ("x", 1, 1), ("x", 1, 2), ("y", 1, 0),
        ),
        (
            ("x", 1, 3), ("z", 2, 0),
        ),
        (
            ("y", 1, 1), ("x", 1, 4), ("y", 1, 2), ("z", 2, 1),
        ),
        (
            ("y", 1, 3), ("d", 1, 0), ("z", 2, 2), ("y", 1, 4), ("z", 2, 3),
        ),
        (
            ("x", 2, 0), ("d", 1, 3), ("z", 2, 4),
        ),
        (
            ("d", 1, 1), ("y", 2, 0), ("d", 1, 4), ("d", 1, 2),
        ),
        (
            ("z", 3, 0), ("y", 2, 1), ("x", 2, 1), ("z", 3, 1), ("y", 2, 2),
        ),
        (
            ("x", 2, 2), ("z", 3, 2), ("y", 2, 3), ("x", 2, 3),
        ),
        (
            ("z", 3, 3), ("y", 2, 4), ("x", 2, 4), ("z", 3, 4),
        ),
        (
            ("d", 2, 0), ("y", 3, 0),
        ),
        (
            ("x", 3, 0), ("y", 3, 1), ("y", 3, 2), ("d", 2, 1),
        ),
        (
            ("d", 2, 3), ("x", 3, 1), ("y", 3, 3),
        ),
        (
            ("d", 2, 2), ("d", 2, 4), ("y", 3, 4), ("x", 3, 2), ("x", 3, 3),
        ),
        (
            ("x", 3, 4),
        ),
        (
            ("d", 3, 0), ("d", 3, 3), ("d", 3, 1),
        ),
        (
            ("d", 3, 2), ("d", 3, 4),
        ),
        (),
        (),
        (),
        (),
        (),
        (),
        (),
        (),
        (),
    ),
    (
        (),
        (
            ("g", 1, 0), ("g", 3, 0), ("g", 2, 0), ("y", 0, 0), ("y", 0, 1), ("y", 0, 2), ("y", 0, 3), ("d", 0, 0),
            ("y", 0, 4), ("d", 0, 1), ("z", 1, 0), ("d", 0, 2), ("z", 1, 1), ("z", 1, 2), ("h", 0, 0), ("z", 1, 3),
            ("x", 1, 0), ("z", 2, 0), ("d", 0, 3), ("z", 1, 4),
        ),
        (
            ("d", 0, 4), ("x", 1, 1), ("z", 2, 1), ("x", 1, 2), ("z", 2, 2), ("y", 1, 0),
        ),
        (
            ("x", 1, 3), ("z", 2, 3),
        ),
        (
            ("y", 1, 1), ("z", 2, 4), ("x", 2, 0), ("y", 1, 2),
        ),
        (
            ("x", 1, 4), ("z", 3, 0), ("y", 1, 3), ("x", 2, 1), ("z", 3, 1),
        ),
        (
            ("y", 2, 0), ("x", 2, 2), ("z", 3, 2), ("y", 1, 4),
        ),
        (
            ("z", 3, 3), ("d", 1, 0), ("y", 2, 1), ("z", 3, 4), ("x", 2, 3),
        ),
        (
            ("y", 2, 2), ("d", 1, 3), ("d", 1, 1), ("y", 2, 3), ("x", 2, 4), ("y", 2, 4), ("d", 1, 2), ("d", 1, 4),
            ("x", 3, 0),
        ),
        (
            ("y", 3, 0), ("x", 3, 1),
        ),
        (
            ("y", 3, 1), ("d", 2, 0), ("y", 3, 2),
        ),
        (
            ("x", 3, 2), ("y", 3, 3), ("x", 3, 3), ("y", 3, 4),
        ),
        (
            ("d", 2, 3), ("d", 2, 1), ("d", 2, 4),
        ),
        (
            ("x", 3, 4), ("d", 3, 3), ("d", 2, 2),
        ),
        (
            ("d", 3, 0),
        ),
        (
            ("d", 3, 1),
        ),
        (
            ("d", 3, 4), ("d", 3, 2),
        ),
        (),
        (),
        (),
        (),
        (),
        (),
        (),
        (),
        (),
        (),
    ),
)


class Sends:
    def __init__(self, sems):
        self.sems, self.made = sems, {}

    def start(self, key, src, dst, arrived, device, cond=None):
        if key not in self.made:
            index = len(self.made)

            def make():
                return pltpu.make_async_remote_copy(
                    src_ref=src(), dst_ref=dst(), send_sem=self.sems.at[index], recv_sem=arrived(),
                    device_id=device, device_id_type=MESH,
                )

            self.made[key] = make, cond
        make, cond = self.made[key]
        if cond is None:
            make().start()
        else:
            pl.when(cond)(lambda: make().start())

    def finish(self):
        for make, cond in self.made.values():
            if cond is None:
                make().wait_send()
            else:
                pl.when(cond)(lambda make=make: make().wait_send())


def cuts(width):
    return [(start, min(start + STEP, QUERIES * width)) for start in range(0, QUERIES * width, STEP)]


def layer_at(step, z):
    table = ((0, 1, 2, 3), (1, 0, 2, 3), (2, 3, 1, 0), (3, 2, 1, 0))
    out = jnp.int32(table[0][step])
    for row in range(1, LAYERS):
        out = jnp.where(z == row, jnp.int32(table[row][step]), out)
    return out


def gather_kernel(
    order, acts_ref, grads_ref, ids_ref, blocks_ref, own_ref, eig_ref,
    out_ref,
    acc_ref, g_ref, gr, ac, idb, ra, wide, turned, eigb, scaled, backs, rgt,
    send_sems, local_sems, g_sems, grz_sems, gry_sems, grc_sems, many_sems,
):
    own_tokens = ids_ref.shape[0]
    units, cols = own_ref.shape
    width = ac.shape[1]
    half = units // 2
    edges = [half * e // 1024 // 16 * 16 for e in PIECES] + [half]
    parts = range(len(PIECES))
    count = len(PIECES)
    deep = 4 * cols
    n = 4 * LAYERS
    x, s = lax.axis_index("groups"), lax.axis_index("seq")
    z, y, c = s // 4, s // 2 % 2, s % 2
    layers = [layer_at(t, z) for t in range(LAYERS)]

    def dev(zz, yy, cc):
        return (x, (zz * 2 + yy) * 2 + cc)

    x_mate, y_mate, c_mate = (1 - x, s), dev(z, 1 - y, c), dev(z, y, 1 - c)

    def token_rows(zz, yy, cc, count=1):
        start = ((yy * 2 + cc) * LAYERS + zz) * own_tokens
        return pl.ds(pl.multiple_of(start, own_tokens), count * own_tokens)

    def piece(slot, p):
        side, i = p
        return g_ref.at[slot, pl.ds(pl.multiple_of(side * half + edges[i], 16), edges[i + 1] - edges[i])]

    def slot_of(zz, yy, cc):
        return (zz * 2 + yy) * 2 + cc

    me = slot_of(z, y, c)
    column_slots = [slot_of(layer, y, c) for layer in layers]
    other_slots = [slot_of(layer, 1 - y, c) for layer in layers]
    core_slots = [[slot_of(layer, yy, 1 - c) for yy in (y, 1 - y)] for layer in layers]
    onward = [jnp.where(layer < z, z + 1, z - 1) for layer in layers]
    goes_on = [jnp.logical_and(to >= 0, to < LAYERS) for to in onward]
    beyond = [dev(to, y, c) for to in onward]
    halves = [(x, i) for i in parts]
    mate_halves = [(1 - x, i) for i in parts]
    mine = token_rows(z, y, c)

    local = [
        pltpu.make_async_copy(own_ref, g_ref.at[me], local_sems.at[0]),
        pltpu.make_async_copy(grads_ref, gr.at[mine], local_sems.at[1]),
        pltpu.make_async_copy(acts_ref.at[:, pl.ds(pl.multiple_of(s * width, 128), width)], ac.at[mine], local_sems.at[2]),
        pltpu.make_async_copy(ids_ref, idb.at[mine], local_sems.at[3]),
    ]
    for copy in local:
        copy.start()

    def eig_copy(t):
        at = pl.ds(pl.multiple_of(layers[t] * deep, deep), deep)
        return pltpu.make_async_copy(eig_ref.at[at], eigb.at[t % 2], local_sems.at[4 + t % 2])

    eig_copy(0).start()
    eig_copy(1).start()

    barrier = pltpu.get_barrier_semaphore()
    peers = [(x, lax.rem(s + k, n)) for k in range(1, n)]
    for peer in peers + [x_mate]:
        pl.semaphore_signal(barrier, inc=1, device_id=peer, device_id_type=MESH)
    pl.semaphore_wait(barrier, n)

    sends = Sends(send_sems)

    def send_grads(key, at, arrived, device):
        sends.start(("grads", *key), lambda: gr.at[at], lambda: gr.at[at], arrived, device)

    def send_piece(to, key, slot, p, device, cond=None):
        sends.start(
            (to, *key), lambda: piece(slot, p), lambda: piece(slot, p),
            lambda: g_sems.at[slot, p[0] * count + p[1]], device, cond,
        )

    def wait_piece(slot, p):
        pltpu.make_async_copy(piece(slot, p), piece(slot, p), g_sems.at[slot, p[0] * count + p[1]]).wait()

    local[1].wait()
    for t in range(1, LAYERS):
        send_grads(("z", t), mine, lambda: grz_sems.at[z], dev(layers[t], y, c))
    send_grads(("y", 0), mine, lambda: gry_sems.at[z], y_mate)
    for k, peer in enumerate(peers):
        sends.start(("ids", k), lambda: ids_ref, lambda: idb.at[mine], lambda: many_sems.at[0], peer)
    for k, peer in enumerate(peers):
        at = pl.ds(pl.multiple_of(peer[1] * width, 128), width)
        sends.start(("acts", k), lambda at=at: acts_ref.at[:, at], lambda: ac.at[mine], lambda: many_sems.at[1], peer)
    local[0].wait()
    for i in parts:
        send_piece("y", (0, i), me, halves[i], y_mate)
        send_piece("up", (0, i), me, halves[i], dev(z + 1, y, c), z < LAYERS - 1)
        send_piece("down", (0, i), me, halves[i], dev(z - 1, y, c), z > 0)
    for i in parts:
        send_piece("core", ("z", 0, i), me, halves[i], c_mate)
        send_piece("core", ("x", 0, i), me, mate_halves[i], c_mate)

    def from_y(t, i):
        wait_piece(other_slots[t], halves[i])
        if i < count - ACROSS:
            send_piece("x", ("y", t, i), other_slots[t], halves[i], x_mate)
        send_piece("core", ("y", t, i), other_slots[t], halves[i], c_mate)

    def from_z(t, i):
        wait_piece(column_slots[t], halves[i])
        send_piece("on", (t, i), column_slots[t], halves[i], beyond[t], goes_on[t])
        send_piece("x", ("z", t, i), column_slots[t], halves[i], x_mate)
        send_piece("y", (t, i), column_slots[t], halves[i], y_mate)
        send_piece("core", ("z", t, i), column_slots[t], halves[i], c_mate)

    def from_x(t, i):
        wait_piece(column_slots[t], mate_halves[i])
        if i >= count - ACROSS:
            send_piece("y", ("x", t, i), column_slots[t], mate_halves[i], y_mate)
        send_piece("core", ("x", t, i), column_slots[t], mate_halves[i], c_mate)

    def diagonal(t, i):
        wait_piece(other_slots[t], mate_halves[i])
        send_piece("core", ("d", t, i), other_slots[t], mate_halves[i], c_mate)

    def from_core(t):
        for slot in core_slots[t]:
            for p in halves + mate_halves:
                wait_piece(slot, p)

    def wait_grads(at, sem):
        pltpu.make_async_copy(gr.at[at], gr.at[at], sem).wait()

    own_rows = [token_rows(layer, y, c) for layer in layers]
    column, other = token_rows(0, y, c, LAYERS), token_rows(0, 1 - y, c, LAYERS)

    def grads_along(t, last):
        wait_grads(own_rows[t], grz_sems.at[layers[t]])
        send_grads(("y", t), own_rows[t], lambda: gry_sems.at[layers[t]], y_mate)
        if last:
            send_grads(("core", 0), column, lambda: grc_sems.at[0], c_mate)
            for i in range(count - ACROSS, count):
                send_piece("y", ("x", 0, i), me, mate_halves[i], y_mate)

    def grads_across():
        for layer in range(LAYERS):
            wait_grads(token_rows(layer, 1 - y, c), gry_sems.at[layer])
        send_grads(("core", 1), other, lambda: grc_sems.at[1], c_mate)

    doers = {"x": from_x, "y": from_y, "z": from_z, "d": diagonal}
    at_end = jnp.logical_or(z == 0, z == LAYERS - 1)

    def pass_on(now):
        for place, here in enumerate((at_end, jnp.logical_not(at_end))):
            table = EVENTS[place]
            along = [event for todo in table for event in todo if event[0] == "g"]

            def body(todo=table[now], along=along):
                for kind, t, i in todo:
                    if kind == "g":
                        grads_along(t, (kind, t, i) == along[-1])
                    elif kind == "h":
                        grads_across()
                    else:
                        doers[kind](t, i)

            if table[now]:
                pl.when(here)(body)

    pass_on(0)
    wide[...] = jnp.zeros_like(wide)
    turned[...] = jnp.zeros_like(turned)
    for b in range(blocks_ref.shape[0]):
        at = slice(b * order, (b + 1) * order)
        wide[at, at] = blocks_ref[b]
        turned[at, at] = blocks_ref[b].T

    def rotate_grads(t):
        base = layers[t] * 4
        both = jnp.concatenate([g_ref[base + i] for i in range(4)], axis=1)
        rg = jnp.dot(gr[...], both, preferred_element_type=jnp.float32).astype(jnp.bfloat16)
        rgt[...] = rg.T

    def invert(t):
        eig_copy(t).wait()
        eigb[t % 2] = 1.0 / eigb[t % 2]

    def scale_back(t):
        if t > 1:
            invert(t)
        for start, stop in cuts(width):
            moments = jnp.dot(rgt[...], ra[:, start:stop], preferred_element_type=jnp.float32)
            for lane in range(start, stop, LANES):
                value = moments[:, lane - start : lane - start + LANES]
                inverse = eigb[t % 2, :, lane % width : lane % width + LANES]
                scaled[:, lane : lane + LANES] = (value * inverse).astype(jnp.bfloat16)
        for query in range(QUERIES):
            for start, stop, low, high in bands(width, order):
                backs[:, query * width + start : query * width + stop] = jnp.dot(
                    scaled[:, query * width + low : query * width + high], turned[low:high, start:stop],
                    preferred_element_type=jnp.float32,
                ).astype(jnp.bfloat16)
        if t + 2 < LAYERS:
            eig_copy(t + 2).start()

    def accumulate(t, first):
        base = layers[t] * 4

        def body(r, carry):
            at = pl.ds(pl.multiple_of(r * TALL, TALL), TALL)
            left = jnp.concatenate([g_ref[base + i, at, :] for i in range(4)], axis=1)
            for start, stop in cuts(width):
                term = jnp.dot(left, backs[:, start:stop], preferred_element_type=jnp.float32)
                if t > 0:
                    term = acc_ref[at, start:stop] + term
                if t < LAYERS - 1:
                    acc_ref[at, start:stop] = term
                else:
                    for query in range(start // width, (stop - 1) // width + 1):
                        low, high = max(start, query * width), min(stop, (query + 1) * width)
                        out_ref[query, at, low - query * width : high - query * width] = term[
                            :, low - start : high - start
                        ].astype(jnp.bfloat16)
            for k in range(units // TALL):
                if any(table[first + k] for table in EVENTS):
                    pl.when(r == k)(functools.partial(pass_on, first + k))
            return carry

        lax.fori_loop(0, units // TALL, body, 0)

    invert(0)
    invert(1)
    pass_on(1)
    local[2].wait()
    local[3].wait()
    others = pl.ds(0, (n - 1) * own_tokens)
    pltpu.make_async_copy(idb.at[others], idb.at[others], many_sems.at[0]).wait()
    pltpu.make_async_copy(ac.at[others], ac.at[others], many_sems.at[1]).wait()
    ids = idb[...][:, 0:1]
    for start, stop, low, high in bands(width, order):
        turned_act = jnp.dot(ac[:, low:high], wide[low:high, start:stop], preferred_element_type=jnp.float32)
        turned_act = turned_act.astype(jnp.bfloat16)
        for query in range(QUERIES):
            ra[:, query * width + start : query * width + stop] = turned_act * (ids == query).astype(jnp.bfloat16)

    pass_on(2)
    for i, yy in enumerate((y, 1 - y)):
        wait_grads(token_rows(0, yy, 1 - c, LAYERS), grc_sems.at[i])
    from_core(0)
    rotate_grads(0)
    pass_on(3)
    now = 4
    for t in range(LAYERS):
        if t > 0:
            from_core(t)
            rotate_grads(t)
            pass_on(now)
            now += 1
        scale_back(t)
        pass_on(now)
        accumulate(t, now + 1)
        now += 1 + units // TALL
    sends.finish()


def square_shards(n, activations, out_grads, query_ids, act_basis, grad_basis, eigenvalues):
    own_tokens = activations.shape[0]
    blocks, order = act_basis.shape[:2]
    units, cols = grad_basis.shape
    width = blocks * order
    tokens = own_tokens * n
    deep = 4 * cols
    ids = jnp.broadcast_to(query_ids[:, None], (own_tokens, LANES))
    hbm, vmem = pl.BlockSpec(memory_space=pltpu.HBM), pl.BlockSpec(memory_space=pltpu.VMEM)
    return pl.pallas_call(
        functools.partial(gather_kernel, order),
        out_shape=pltpu.VMEM((QUERIES, units, width), jnp.bfloat16),
        in_specs=[hbm, hbm, hbm, vmem, hbm, hbm],
        out_specs=vmem,
        scratch_shapes=[
            pltpu.VMEM((units, QUERIES * width), jnp.float32),
            pltpu.VMEM((n, units, cols), jnp.bfloat16),
            pltpu.VMEM((tokens, units), jnp.bfloat16),
            pltpu.VMEM((tokens, width), jnp.bfloat16),
            pltpu.VMEM((tokens, LANES), jnp.int32),
            pltpu.VMEM((tokens, QUERIES * width), jnp.bfloat16),
            pltpu.VMEM((width, width), jnp.bfloat16),
            pltpu.VMEM((width, width), jnp.bfloat16),
            pltpu.VMEM((2, deep, width), jnp.float32),
            pltpu.VMEM((deep, QUERIES * width), jnp.bfloat16),
            pltpu.VMEM((deep, QUERIES * width), jnp.bfloat16),
            pltpu.VMEM((deep, tokens), jnp.bfloat16),
            pltpu.SemaphoreType.DMA((288,)),
            pltpu.SemaphoreType.DMA((6,)),
            pltpu.SemaphoreType.DMA((n, 2 * len(PIECES))),
            pltpu.SemaphoreType.DMA((LAYERS,)),
            pltpu.SemaphoreType.DMA((LAYERS,)),
            pltpu.SemaphoreType.DMA((2,)),
            pltpu.SemaphoreType.DMA((2,)),
        ],
        compiler_params=pltpu.CompilerParams(
            collective_id=0, has_side_effects=True, vmem_limit_bytes=51 * 2**20
        ),
        cost_estimate=pl.CostEstimate(
            flops=2 * QUERIES * units * units * width, bytes_accessed=4 * units * width, transcendentals=0
        ),
        name="gather",
    )(activations, out_grads, ids, act_basis, grad_basis, eigenvalues)


def shards(groups, n, activations, out_grads, query_ids, act_basis, grad_basis, eigenvalues):
    args = activations, out_grads, query_ids, act_basis, grad_basis, eigenvalues
    units, cols = grad_basis.shape
    width = act_basis.shape[0] * act_basis.shape[1]
    if groups == 2 and n == 4 * LAYERS and cols % LANES == 0 and width % LANES == 0 and units == 4 * TALL:
        return square_shards(n, *args)
    return ring_shards(groups, n, *args)


def solution(mesh):
    return jax.shard_map(
        functools.partial(shards, mesh.shape["groups"], mesh.shape["seq"]),
        mesh=mesh,
        in_specs=(
            P(("groups", "seq"), None),
            P(("groups", "seq"), None),
            P(("groups", "seq")),
            P("seq", None, None),
            P(None, "seq"),
            P(None, "seq"),
        ),
        out_specs=P("groups", None, "seq"),
        check_vma=False,
    )
```

```python
import functools

import jax
import jax.numpy as jnp
from jax import lax
from jax.experimental import pallas as pl
from jax.experimental.pallas import tpu as pltpu
from jax.sharding import PartitionSpec as P

QUERIES = 3
LANES = 128
TILE = 256
TALL = 512
STEP = 768


def bands(width, order):
    out = []
    for start in range(0, width, TILE):
        stop = min(start + TILE, width)
        low = start // order * order // LANES * LANES
        high = min(width, -(-(((stop - 1) // order + 1) * order) // LANES) * LANES)
        out.append((start, stop, low, high))
    return out


def back_kernel(order, basis_ref, grads_ref, act_ref, ids_ref, eig_ref, turn_ref, out_ref):
    rotated = jnp.dot(grads_ref[...], basis_ref[...], preferred_element_type=jnp.float32)
    rotated = rotated.astype(jnp.bfloat16)
    act = act_ref[...]
    ids = ids_ref[...]
    for query in range(QUERIES):
        selected = act * (ids == query).astype(jnp.bfloat16)
        moments = lax.dot_general(
            rotated, selected, (((0,), (0,)), ((), ())), preferred_element_type=jnp.float32
        )
        scaled = (moments / eig_ref[...]).astype(jnp.bfloat16)
        for start, stop, low, high in bands(act.shape[1], order):
            out_ref[query, :, start:stop] = jnp.dot(
                scaled[:, low:high], turn_ref[low:high, start:stop], preferred_element_type=jnp.float32
            ).astype(jnp.bfloat16)


def final_kernel(chunks, *refs):
    basis, back, out_ref = refs[:chunks], refs[chunks : 2 * chunks], refs[-1]
    total = None
    for g, b in zip(basis, back):
        term = jnp.dot(g[...], b[0], preferred_element_type=jnp.float32)
        total = term if total is None else total + term
    out_ref[0] = total.astype(jnp.bfloat16)


def ring_shards(groups, n, activations, out_grads, query_ids, act_basis, grad_basis, eigenvalues):
    own_tokens = activations.shape[0]
    blocks, order = act_basis.shape[:2]
    units, cols = grad_basis.shape
    width = blocks * order
    tokens = own_tokens * n
    outer = n // 4
    me, group = lax.axis_index("seq"), lax.axis_index("groups")
    z, y, c = me // 4, me // 2 % 2, me % 2

    ring = [(i, (i + 4) % n) for i in range(n)]
    side = [(i, i ^ 2) for i in range(n)]
    core = [(i, i ^ 1) for i in range(n)]

    pieces = [grad_basis]
    for _ in range(outer - 1):
        pieces.append(lax.ppermute(pieces[-1], "seq", ring))
    chunks, eigs = [], []
    for step, piece in enumerate(pieces):
        if groups == 2 and units % 32 == 0:
            half = units // 2
            sent = lax.dynamic_slice_in_dim(piece, group * half, half, axis=0)
            mine = lax.ppermute(sent, "seq", side)
            theirs = lax.ppermute(mine, "groups", [(0, 1), (1, 0)])
            first = group == 0
            other = jnp.concatenate(
                [jnp.where(first, mine, theirs), jnp.where(first, theirs, mine)], axis=0
            )
        else:
            other = lax.ppermute(piece, "seq", side)
        pair = jnp.concatenate([piece, other], axis=1)
        chunks.append(jnp.concatenate([pair, lax.ppermute(pair, "seq", core)], axis=1))
        level = (z - step) % outer * 4
        origins = [level + yy * 2 + cc for cc in (c, 1 - c) for yy in (y, 1 - y)]
        eigs.append(
            jnp.concatenate(
                [lax.dynamic_slice_in_dim(eigenvalues, o * cols, cols, axis=0) for o in origins], axis=0
            )
        )

    ids = jnp.broadcast_to(query_ids.astype(jnp.bfloat16)[:, None, None], (own_tokens, n, LANES))
    every = jnp.broadcast_to(out_grads[:, None, :], (own_tokens, n, units))
    sent = jnp.concatenate([activations.reshape(own_tokens, n, width), ids, every], axis=2)
    columns = lax.all_to_all(
        jnp.transpose(sent, (1, 0, 2)), "seq", split_axis=0, concat_axis=0, tiled=True
    ).reshape(tokens, width + LANES + units)
    token_query = columns[:, width : width + 1].astype(jnp.float32)
    grads = columns[:, width + LANES :]

    wide = jnp.concatenate(
        [
            jnp.pad(act_basis[b], ((0, 0), (b * order, width - (b + 1) * order)))
            for b in range(blocks)
        ],
        axis=0,
    )
    turned = wide.T
    act = jnp.dot(columns[:, :width], wide, preferred_element_type=jnp.float32).astype(jnp.bfloat16)

    chunk_cols = 4 * cols
    backs = [
        pl.pallas_call(
            functools.partial(back_kernel, order),
            out_shape=jax.ShapeDtypeStruct((QUERIES, chunk_cols, width), jnp.bfloat16),
            in_specs=[pl.BlockSpec(memory_space=pltpu.VMEM)] * 6,
            out_specs=pl.BlockSpec(memory_space=pltpu.VMEM),
            compiler_params=pltpu.CompilerParams(vmem_limit_bytes=40 * 2**20),
            cost_estimate=pl.CostEstimate(
                flops=2 * chunk_cols * (tokens * units + QUERIES * width * (tokens + width // 2)),
                bytes_accessed=2 * units * (chunk_cols + tokens) + 10 * chunk_cols * width,
                transcendentals=0,
            ),
            name="back",
        )(chunk, grads, act, token_query, eig, turned)
        for chunk, eig in zip(chunks, eigs)
    ]

    rows = min(units, 512)
    return pl.pallas_call(
        functools.partial(final_kernel, outer),
        grid=(QUERIES, units // rows),
        out_shape=jax.ShapeDtypeStruct((QUERIES, units, width), jnp.bfloat16),
        in_specs=[pl.BlockSpec((rows, chunk_cols), lambda q, r: (r, 0))] * outer
        + [pl.BlockSpec((1, chunk_cols, width), lambda q, r: (q, 0, 0))] * outer,
        out_specs=pl.BlockSpec((1, rows, width), lambda q, r: (q, r, 0)),
        compiler_params=pltpu.CompilerParams(vmem_limit_bytes=40 * 2**20),
        cost_estimate=pl.CostEstimate(
            flops=2 * QUERIES * units * units * width,
            bytes_accessed=2 * units * units + 4 * QUERIES * units * width,
            transcendentals=0,
        ),
        name="final",
    )(*chunks, *backs)


MESH = pl.DeviceIdType.MESH
LAYERS = 4
PIECES = (0, 256, 512, 768)
ACROSS = 1
EVENTS = (
    (
        (),
        (
            ("g", 1, 0), ("g", 3, 0), ("g", 2, 0), ("y", 0, 0), ("y", 0, 1), ("y", 0, 2), ("d", 0, 0), ("y", 0, 3),
            ("d", 0, 1), ("z", 1, 0), ("d", 0, 2), ("z", 1, 1), ("z", 1, 2), ("h", 0, 0), ("x", 1, 0), ("z", 1, 3),
        ),
        (
            ("d", 0, 3), ("x", 1, 1), ("y", 1, 0), ("x", 1, 2),
        ),
        (
            ("y", 1, 1), ("z", 2, 0),
        ),
        (
            ("x", 1, 3), ("y", 1, 2), ("z", 2, 1),
        ),
        (
            ("d", 1, 0), ("y", 1, 3),
        ),
        (
            ("d", 1, 1), ("z", 2, 2), ("y", 2, 0), ("x", 2, 0),
        ),
        (
            ("z", 2, 3), ("d", 1, 3), ("d", 1, 2), ("y", 2, 1),
        ),
        (
            ("z", 3, 0), ("x", 2, 1), ("z", 3, 1),
        ),
        (
            ("y", 2, 2), ("x", 2, 2), ("z", 3, 2),
        ),
        (
            ("y", 2, 3), ("d", 2, 0), ("z", 3, 3),
        ),
        (
            ("x", 2, 3), ("y", 3, 0),
        ),
        (
            ("d", 2, 1), ("y", 3, 1),
        ),
        (
            ("x", 3, 0), ("y", 3, 2), ("x", 3, 1), ("y", 3, 3),
        ),
        (
            ("d", 2, 2), ("d", 2, 3), ("x", 3, 2),
        ),
        (
            ("x", 3, 3),
        ),
        (
            ("d", 3, 0),
        ),
        (
            ("d", 3, 1), ("d", 3, 3), ("d", 3, 2),
        ),
        (),
        (),
        (),
        (),
        (),
        (),
        (),
        (),
        (),
    ),
    (
        (),
        (
            ("g", 1, 0), ("g", 3, 0), ("g", 2, 0), ("y", 0, 0), ("y", 0, 1), ("y", 0, 2), ("d", 0, 0), ("y", 0, 3),
            ("d", 0, 1), ("z", 1, 0), ("d", 0, 2), ("z", 1, 1), ("z", 1, 2), ("h", 0, 0), ("x", 1, 0), ("z", 2, 0),
            ("z", 1, 3),
        ),
        (
            ("d", 0, 3), ("x", 1, 1), ("z", 2, 1), ("y", 1, 0), ("x", 1, 2),
        ),
        (
            ("z", 2, 2), ("y", 1, 1),
        ),
        (
            ("x", 2, 0), ("z", 2, 3), ("y", 1, 2), ("x", 1, 3),
        ),
        (
            ("z", 3, 0), ("y", 2, 0), ("x", 2, 1), ("z", 3, 1),
        ),
        (
            ("y", 1, 3), ("d", 1, 0), ("z", 3, 2),
        ),
        (
            ("y", 2, 1), ("x", 2, 2), ("z", 3, 3), ("y", 2, 2),
        ),
        (
            ("d", 1, 1), ("y", 2, 3), ("x", 2, 3), ("d", 1, 3), ("d", 1, 2), ("y", 3, 0),
        ),
        (
            ("x", 3, 0), ("y", 3, 1),
        ),
        (
            ("d", 2, 0), ("y", 3, 2),
        ),
        (
            ("x", 3, 1), ("y", 3, 3), ("x", 3, 2),
        ),
        (
            ("d", 2, 3), ("d", 2, 1),
        ),
        (
            ("x", 3, 3),
        ),
        (
            ("d", 2, 2), ("d", 3, 0),
        ),
        (
            ("d", 3, 1), ("d", 3, 3),
        ),
        (
            ("d", 3, 2),
        ),
        (),
        (),
        (),
        (),
        (),
        (),
        (),
        (),
        (),
        (),
    ),
)


class Sends:
    def __init__(self, sems):
        self.sems, self.made = sems, {}

    def start(self, key, src, dst, arrived, device, cond=None):
        if key not in self.made:
            index = len(self.made)

            def make():
                return pltpu.make_async_remote_copy(
                    src_ref=src(), dst_ref=dst(), send_sem=self.sems.at[index], recv_sem=arrived(),
                    device_id=device, device_id_type=MESH,
                )

            self.made[key] = make, cond
        make, cond = self.made[key]
        if cond is None:
            make().start()
        else:
            pl.when(cond)(lambda: make().start())

    def finish(self):
        for make, cond in self.made.values():
            if cond is None:
                make().wait_send()
            else:
                pl.when(cond)(lambda make=make: make().wait_send())


def cuts(width):
    return [(start, min(start + STEP, QUERIES * width)) for start in range(0, QUERIES * width, STEP)]


def layer_at(step, z):
    table = ((0, 1, 2, 3), (1, 0, 2, 3), (2, 3, 1, 0), (3, 2, 1, 0))
    out = jnp.int32(table[0][step])
    for row in range(1, LAYERS):
        out = jnp.where(z == row, jnp.int32(table[row][step]), out)
    return out


def gather_kernel(
    order, acts_ref, grads_ref, ids_ref, blocks_ref, own_ref, eig_ref,
    out_ref,
    acc_ref, g_ref, gr, ac, idb, ra, wide, turned, eigb, scaled, backs, rgt,
    send_sems, local_sems, g_sems, grz_sems, gry_sems, grc_sems, many_sems,
):
    own_tokens = ids_ref.shape[0]
    units, cols = own_ref.shape
    width = ac.shape[1]
    half = units // 2
    edges = [half * e // 1024 // 16 * 16 for e in PIECES] + [half]
    parts = range(len(PIECES))
    count = len(PIECES)
    deep = 4 * cols
    n = 4 * LAYERS
    x, s = lax.axis_index("groups"), lax.axis_index("seq")
    z, y, c = s // 4, s // 2 % 2, s % 2
    layers = [layer_at(t, z) for t in range(LAYERS)]

    def dev(zz, yy, cc):
        return (x, (zz * 2 + yy) * 2 + cc)

    x_mate, y_mate, c_mate = (1 - x, s), dev(z, 1 - y, c), dev(z, y, 1 - c)

    def token_rows(zz, yy, cc, count=1):
        start = ((yy * 2 + cc) * LAYERS + zz) * own_tokens
        return pl.ds(pl.multiple_of(start, own_tokens), count * own_tokens)

    def piece(slot, p):
        side, i = p
        return g_ref.at[slot, pl.ds(pl.multiple_of(side * half + edges[i], 16), edges[i + 1] - edges[i])]

    def slot_of(zz, yy, cc):
        return (zz * 2 + yy) * 2 + cc

    me = slot_of(z, y, c)
    column_slots = [slot_of(layer, y, c) for layer in layers]
    other_slots = [slot_of(layer, 1 - y, c) for layer in layers]
    core_slots = [[slot_of(layer, yy, 1 - c) for yy in (y, 1 - y)] for layer in layers]
    onward = [jnp.where(layer < z, z + 1, z - 1) for layer in layers]
    goes_on = [jnp.logical_and(to >= 0, to < LAYERS) for to in onward]
    beyond = [dev(to, y, c) for to in onward]
    halves = [(x, i) for i in parts]
    mate_halves = [(1 - x, i) for i in parts]
    mine = token_rows(z, y, c)

    local = [
        pltpu.make_async_copy(own_ref, g_ref.at[me], local_sems.at[0]),
        pltpu.make_async_copy(grads_ref, gr.at[mine], local_sems.at[1]),
        pltpu.make_async_copy(acts_ref.at[:, pl.ds(pl.multiple_of(s * width, 128), width)], ac.at[mine], local_sems.at[2]),
        pltpu.make_async_copy(ids_ref, idb.at[mine], local_sems.at[3]),
    ]
    for copy in local:
        copy.start()

    def eig_copy(t):
        at = pl.ds(pl.multiple_of(layers[t] * deep, deep), deep)
        return pltpu.make_async_copy(eig_ref.at[at], eigb.at[t % 2], local_sems.at[4 + t % 2])

    eig_copy(0).start()
    eig_copy(1).start()

    barrier = pltpu.get_barrier_semaphore()
    peers = [(x, lax.rem(s + k, n)) for k in range(1, n)]
    for peer in peers + [x_mate]:
        pl.semaphore_signal(barrier, inc=1, device_id=peer, device_id_type=MESH)
    pl.semaphore_wait(barrier, n)

    sends = Sends(send_sems)

    def send_grads(key, at, arrived, device):
        sends.start(("grads", *key), lambda: gr.at[at], lambda: gr.at[at], arrived, device)

    def send_piece(to, key, slot, p, device, cond=None):
        sends.start(
            (to, *key), lambda: piece(slot, p), lambda: piece(slot, p),
            lambda: g_sems.at[slot, p[0] * count + p[1]], device, cond,
        )

    def wait_piece(slot, p):
        pltpu.make_async_copy(piece(slot, p), piece(slot, p), g_sems.at[slot, p[0] * count + p[1]]).wait()

    local[1].wait()
    for t in range(1, LAYERS):
        send_grads(("z", t), mine, lambda: grz_sems.at[z], dev(layers[t], y, c))
    send_grads(("y", 0), mine, lambda: gry_sems.at[z], y_mate)
    for k, peer in enumerate(peers):
        sends.start(("ids", k), lambda: ids_ref, lambda: idb.at[mine], lambda: many_sems.at[0], peer)
    for k, peer in enumerate(peers):
        at = pl.ds(pl.multiple_of(peer[1] * width, 128), width)
        sends.start(("acts", k), lambda at=at: acts_ref.at[:, at], lambda: ac.at[mine], lambda: many_sems.at[1], peer)
    local[0].wait()
    for i in parts:
        send_piece("y", (0, i), me, halves[i], y_mate)
        send_piece("up", (0, i), me, halves[i], dev(z + 1, y, c), z < LAYERS - 1)
        send_piece("down", (0, i), me, halves[i], dev(z - 1, y, c), z > 0)
    for i in parts:
        send_piece("core", ("z", 0, i), me, halves[i], c_mate)
        send_piece("core", ("x", 0, i), me, mate_halves[i], c_mate)

    def from_y(t, i):
        wait_piece(other_slots[t], halves[i])
        if i < count - ACROSS:
            send_piece("x", ("y", t, i), other_slots[t], halves[i], x_mate)
        send_piece("core", ("y", t, i), other_slots[t], halves[i], c_mate)

    def from_z(t, i):
        wait_piece(column_slots[t], halves[i])
        send_piece("on", (t, i), column_slots[t], halves[i], beyond[t], goes_on[t])
        send_piece("x", ("z", t, i), column_slots[t], halves[i], x_mate)
        send_piece("y", (t, i), column_slots[t], halves[i], y_mate)
        send_piece("core", ("z", t, i), column_slots[t], halves[i], c_mate)

    def from_x(t, i):
        wait_piece(column_slots[t], mate_halves[i])
        if i >= count - ACROSS:
            send_piece("y", ("x", t, i), column_slots[t], mate_halves[i], y_mate)
        send_piece("core", ("x", t, i), column_slots[t], mate_halves[i], c_mate)

    def diagonal(t, i):
        wait_piece(other_slots[t], mate_halves[i])
        send_piece("core", ("d", t, i), other_slots[t], mate_halves[i], c_mate)

    def from_core(t):
        for slot in core_slots[t]:
            for p in halves + mate_halves:
                wait_piece(slot, p)

    def wait_grads(at, sem):
        pltpu.make_async_copy(gr.at[at], gr.at[at], sem).wait()

    own_rows = [token_rows(layer, y, c) for layer in layers]
    column, other = token_rows(0, y, c, LAYERS), token_rows(0, 1 - y, c, LAYERS)

    def grads_along(t, last):
        wait_grads(own_rows[t], grz_sems.at[layers[t]])
        send_grads(("y", t), own_rows[t], lambda: gry_sems.at[layers[t]], y_mate)
        if last:
            send_grads(("core", 0), column, lambda: grc_sems.at[0], c_mate)
            for i in range(count - ACROSS, count):
                send_piece("y", ("x", 0, i), me, mate_halves[i], y_mate)

    def grads_across():
        for layer in range(LAYERS):
            wait_grads(token_rows(layer, 1 - y, c), gry_sems.at[layer])
        send_grads(("core", 1), other, lambda: grc_sems.at[1], c_mate)

    doers = {"x": from_x, "y": from_y, "z": from_z, "d": diagonal}
    at_end = jnp.logical_or(z == 0, z == LAYERS - 1)

    def pass_on(now):
        for place, here in enumerate((at_end, jnp.logical_not(at_end))):
            table = EVENTS[place]
            along = [event for todo in table for event in todo if event[0] == "g"]

            def body(todo=table[now], along=along):
                for kind, t, i in todo:
                    if kind == "g":
                        grads_along(t, (kind, t, i) == along[-1])
                    elif kind == "h":
                        grads_across()
                    else:
                        doers[kind](t, i)

            if table[now]:
                pl.when(here)(body)

    pass_on(0)
    wide[...] = jnp.zeros_like(wide)
    turned[...] = jnp.zeros_like(turned)
    for b in range(blocks_ref.shape[0]):
        at = slice(b * order, (b + 1) * order)
        wide[at, at] = blocks_ref[b]
        turned[at, at] = blocks_ref[b].T

    def rotate_grads(t):
        base = layers[t] * 4
        both = jnp.concatenate([g_ref[base + i] for i in range(4)], axis=1)
        rg = jnp.dot(gr[...], both, preferred_element_type=jnp.float32).astype(jnp.bfloat16)
        rgt[...] = rg.T

    def invert(t):
        eig_copy(t).wait()
        eigb[t % 2] = 1.0 / eigb[t % 2]

    def scale_back(t):
        if t > 1:
            invert(t)
        for start, stop in cuts(width):
            moments = jnp.dot(rgt[...], ra[:, start:stop], preferred_element_type=jnp.float32)
            for lane in range(start, stop, LANES):
                value = moments[:, lane - start : lane - start + LANES]
                inverse = eigb[t % 2, :, lane % width : lane % width + LANES]
                scaled[:, lane : lane + LANES] = (value * inverse).astype(jnp.bfloat16)
        for query in range(QUERIES):
            for start, stop, low, high in bands(width, order):
                backs[:, query * width + start : query * width + stop] = jnp.dot(
                    scaled[:, query * width + low : query * width + high], turned[low:high, start:stop],
                    preferred_element_type=jnp.float32,
                ).astype(jnp.bfloat16)
        if t + 2 < LAYERS:
            eig_copy(t + 2).start()

    def accumulate(t, first):
        base = layers[t] * 4

        def body(r, carry):
            at = pl.ds(pl.multiple_of(r * TALL, TALL), TALL)
            left = jnp.concatenate([g_ref[base + i, at, :] for i in range(4)], axis=1)
            for start, stop in cuts(width):
                term = jnp.dot(left, backs[:, start:stop], preferred_element_type=jnp.float32)
                if t > 0:
                    term = acc_ref[at, start:stop] + term
                if t < LAYERS - 1:
                    acc_ref[at, start:stop] = term
                else:
                    for query in range(start // width, (stop - 1) // width + 1):
                        low, high = max(start, query * width), min(stop, (query + 1) * width)
                        out_ref[query, at, low - query * width : high - query * width] = term[
                            :, low - start : high - start
                        ].astype(jnp.bfloat16)
            for k in range(units // TALL):
                if any(table[first + k] for table in EVENTS):
                    pl.when(r == k)(functools.partial(pass_on, first + k))
            return carry

        lax.fori_loop(0, units // TALL, body, 0)

    invert(0)
    invert(1)
    pass_on(1)
    local[2].wait()
    local[3].wait()
    others = pl.ds(0, (n - 1) * own_tokens)
    pltpu.make_async_copy(idb.at[others], idb.at[others], many_sems.at[0]).wait()
    pltpu.make_async_copy(ac.at[others], ac.at[others], many_sems.at[1]).wait()
    ids = idb[...][:, 0:1]
    for start, stop, low, high in bands(width, order):
        turned_act = jnp.dot(ac[:, low:high], wide[low:high, start:stop], preferred_element_type=jnp.float32)
        turned_act = turned_act.astype(jnp.bfloat16)
        for query in range(QUERIES):
            ra[:, query * width + start : query * width + stop] = turned_act * (ids == query).astype(jnp.bfloat16)

    pass_on(2)
    for i, yy in enumerate((y, 1 - y)):
        wait_grads(token_rows(0, yy, 1 - c, LAYERS), grc_sems.at[i])
    from_core(0)
    rotate_grads(0)
    pass_on(3)
    now = 4
    for t in range(LAYERS):
        if t > 0:
            from_core(t)
            rotate_grads(t)
            pass_on(now)
            now += 1
        scale_back(t)
        pass_on(now)
        accumulate(t, now + 1)
        now += 1 + units // TALL
    sends.finish()


def square_shards(n, activations, out_grads, query_ids, act_basis, grad_basis, eigenvalues):
    own_tokens = activations.shape[0]
    blocks, order = act_basis.shape[:2]
    units, cols = grad_basis.shape
    width = blocks * order
    tokens = own_tokens * n
    deep = 4 * cols
    ids = jnp.broadcast_to(query_ids[:, None], (own_tokens, LANES))
    hbm, vmem = pl.BlockSpec(memory_space=pltpu.HBM), pl.BlockSpec(memory_space=pltpu.VMEM)
    return pl.pallas_call(
        functools.partial(gather_kernel, order),
        out_shape=pltpu.VMEM((QUERIES, units, width), jnp.bfloat16),
        in_specs=[hbm, hbm, hbm, vmem, hbm, hbm],
        out_specs=vmem,
        scratch_shapes=[
            pltpu.VMEM((units, QUERIES * width), jnp.float32),
            pltpu.VMEM((n, units, cols), jnp.bfloat16),
            pltpu.VMEM((tokens, units), jnp.bfloat16),
            pltpu.VMEM((tokens, width), jnp.bfloat16),
            pltpu.VMEM((tokens, LANES), jnp.int32),
            pltpu.VMEM((tokens, QUERIES * width), jnp.bfloat16),
            pltpu.VMEM((width, width), jnp.bfloat16),
            pltpu.VMEM((width, width), jnp.bfloat16),
            pltpu.VMEM((2, deep, width), jnp.float32),
            pltpu.VMEM((deep, QUERIES * width), jnp.bfloat16),
            pltpu.VMEM((deep, QUERIES * width), jnp.bfloat16),
            pltpu.VMEM((deep, tokens), jnp.bfloat16),
            pltpu.SemaphoreType.DMA((288,)),
            pltpu.SemaphoreType.DMA((6,)),
            pltpu.SemaphoreType.DMA((n, 2 * len(PIECES))),
            pltpu.SemaphoreType.DMA((LAYERS,)),
            pltpu.SemaphoreType.DMA((LAYERS,)),
            pltpu.SemaphoreType.DMA((2,)),
            pltpu.SemaphoreType.DMA((2,)),
        ],
        compiler_params=pltpu.CompilerParams(
            collective_id=0, has_side_effects=True, vmem_limit_bytes=51 * 2**20
        ),
        cost_estimate=pl.CostEstimate(
            flops=2 * QUERIES * units * units * width, bytes_accessed=4 * units * width, transcendentals=0
        ),
        name="gather",
    )(activations, out_grads, ids, act_basis, grad_basis, eigenvalues)


def shards(groups, n, activations, out_grads, query_ids, act_basis, grad_basis, eigenvalues):
    args = activations, out_grads, query_ids, act_basis, grad_basis, eigenvalues
    units, cols = grad_basis.shape
    width = act_basis.shape[0] * act_basis.shape[1]
    if groups == 2 and n == 4 * LAYERS and cols % LANES == 0 and width % LANES == 0 and units == 4 * TALL:
        return square_shards(n, *args)
    return ring_shards(groups, n, *args)


def solution(mesh):
    return jax.shard_map(
        functools.partial(shards, mesh.shape["groups"], mesh.shape["seq"]),
        mesh=mesh,
        in_specs=(
            P(("groups", "seq"), None),
            P(("groups", "seq"), None),
            P(("groups", "seq")),
            P("seq", None, None),
            P(None, "seq"),
            P(None, "seq"),
        ),
        out_specs=P("groups", None, "seq"),
        check_vma=False,
    )
```
